256 devices in a mesh: tm: 32 (over y, x, core), grp: 8 (over z).
Axes of the slice: x: 4, y: 4, z: 8, core: 2. Of those that a mesh axis runs over, the one named last changes fastest.
Arguments:
- gate_pre: bfloat16 [2, 16384, 4096], P(None, ('tm', 'grp')), may hold values from 0 to 16
- cand_pre: bfloat16 [2, 16384, 4096], P(None, ('tm', 'grp')), may hold values from -4 to 4
- start_state: float32 [2, 4096], replicated, may hold values from -3 to 3
- mix_gate: float32 [4096], replicated, may hold values from -1.5 to 1.5
- mix_cand: float32 [4096], replicated, may hold values from -1.2 to 1.2
Outputs:
- hidden: bfloat16 [2, 16384, 4096], P(None, ('tm', 'grp'))
The draws below stay inside these ranges and needn't reach their ends.
All inputs are finite; a program needn't handle non-finite values.
Results may differ from the reference program's by a relative error of at most 0.004.
Values may be sent and summed in bfloat16 or wider, within the bound.
No kernel may reach another device: no remote copies, remote signals or barrier semaphores. Data moves between devices by JAX's collectives and lax.ppermute only.
A program may use at most 64 MiB of HBM per device.

```python
import math
import jax
import jax.numpy as jnp
from jax import lax

D = 4096
SEQS = 2
ITERS = 3
LEN = 16384


def draw_gate_pre(key, part):
    keys = [jax.random.fold_in(key, 101 + number) for number in range(7)]
    fast_share = 0.5
    is_fast = jax.random.uniform(keys[0], (D,)) < fast_share
    rate_fast = jnp.exp(jax.random.uniform(keys[1], (D,), jnp.float32, math.log(0.02), math.log(1.0 / 30.0)))
    rate_slow = jnp.exp(jax.random.uniform(keys[2], (D,), jnp.float32, math.log(0.05), 0.0)) / LEN
    rate = jnp.where(is_fast, rate_fast, rate_slow)
    starting_shift = jnp.log(1.0 / rate - 1.0)
    gaussian_perturbation = jnp.clip(0.5 * jax.random.normal(keys[3], (SEQS, LEN, D), jnp.float32), -1.5, 1.5)
    destination_slots = jax.random.randint(keys[4], (SEQS, 1, 4), 0, LEN)
    element_indices = jnp.arange(LEN)[None, :, None]
    span_count = jnp.any(element_indices == destination_slots, axis=2, keepdims=True)
    perturbation_scale = jax.random.uniform(keys[5], (SEQS, LEN, 1), jnp.float32, 0.0, 1.4)
    payload_items = jnp.where(span_count, perturbation_scale, starting_shift[None, None, :] + gaussian_perturbation)
    return payload_items.astype(jnp.bfloat16)


def block_levels(own_key, extent, pieces, smallest, high):
    gain = 1.0
    for axis_at, shards_of in pieces:
        draws = jax.random.uniform(jax.random.fold_in(jax.random.fold_in(own_key, 6), axis_at), (shards_of,), jnp.float32, smallest / len(pieces), high / len(pieces))
        gain = gain * jnp.repeat(jnp.exp(draws), extent[axis_at] // shards_of).reshape((-1,) + (1,) * (len(extent) - 1 - axis_at))
    return gain


def normal_values(own_key, shape, scale, reach, pieces=(), dtype=jnp.bfloat16):
    level = block_levels(own_key, shape, pieces, -0.22, 0.18) if pieces else 1.0
    entries = jax.random.normal(own_key, shape, jnp.float32) * scale * level
    return jnp.minimum(jnp.maximum(entries, -reach), reach).astype(dtype)


def setup_inputs(seed: int = 0) -> dict:
    streams_of = jax.random.split(jax.random.key(seed), 6)
    return {
        "gate_pre": draw_gate_pre(jax.random.fold_in(streams_of[5], 71), 0),
        "cand_pre": normal_values(streams_of[1], (SEQS, LEN, D), 1.0, 4.0, ((1, 256),)),
        "start_state": normal_values(streams_of[2], (SEQS, D), 0.7, 3.0, (), jnp.float32),
        "mix_gate": jnp.clip(jax.random.uniform(streams_of[3], (D,), jnp.float32, -1.5, 1.5), -1.5, 1.5),
        "mix_cand": jnp.clip(jax.random.uniform(streams_of[4], (D,), jnp.float32, -1.2, 1.2), -1.2, 1.2),
    }


def coefficients(gate_in, cand_in, previous, mix_gate, mix_cand):
    forget = jax.nn.sigmoid(gate_in + mix_gate * previous)
    candidate = jnp.tanh(cand_in + mix_cand * previous)
    slopes = forget + (previous - candidate) * forget * (1.0 - forget) * mix_gate + (1.0 - forget) * (1.0 - candidate * candidate) * mix_cand
    offset = forget * previous + (1.0 - forget) * candidate - slopes * previous
    return slopes, offset


def reference(gate_pre, cand_pre, start_state, mix_gate, mix_cand):
    gate_time = jnp.swapaxes(gate_pre, 0, 1)
    cand_time = jnp.swapaxes(cand_pre, 0, 1)
    estimate = jnp.zeros(gate_time.shape, jnp.float32)
    for iteration in range(ITERS):
        def advance(carry, inputs):
            state, before = carry
            gate_row, cand_row, old_row = inputs
            slopes, offset = coefficients(gate_row.astype(jnp.float32), cand_row.astype(jnp.float32), before, mix_gate, mix_cand)
            state = slopes * state + offset
            return (state, old_row), state

        carry_out, estimate = lax.scan(advance, (start_state, start_state), (gate_time, cand_time, estimate))
    return jnp.swapaxes(estimate, 0, 1).astype(jnp.bfloat16)
```

```python
import functools

import jax
import jax.numpy as jnp
from jax import lax
from jax.experimental import pallas as pl
from jax.experimental.pallas import tpu as pltpu
from jax.sharding import PartitionSpec as P

LANES = 128
SUB = 8
GROUP = SUB * LANES
VMEM = pl.BlockSpec(memory_space=pltpu.VMEM)


def sigmoid(x):
    return 0.5 * jnp.tanh(0.5 * x) + 0.5


def coefficients(gate_in, cand_in, previous, mix_gate, mix_cand):
    forget = sigmoid(gate_in + mix_gate * previous)
    candidate = jnp.tanh(cand_in + mix_cand * previous)
    gap = previous - candidate
    kept = forget * gap
    slopes = forget + (1.0 - forget) * (kept * mix_gate + (mix_cand - candidate * candidate * mix_cand))
    offset = candidate + kept - slopes * previous
    return slopes, offset


def coefficients_at_zero(gate_in, cand_in, mix_gate, mix_cand):
    forget = sigmoid(gate_in)
    candidate = jnp.tanh(cand_in)
    kept = forget * candidate
    slopes = forget + (1.0 - forget) * ((mix_cand - candidate * candidate * mix_cand) - kept * mix_gate)
    return slopes, candidate - kept


def first_kernel(seqs, steps, groups, gate_ref, cand_ref, start_ref, mg_ref, mc_ref,
                 slopes_ref, offset_ref, gate_rows_ref, cand_rows_ref, map_ref, gate_tmp, cand_tmp):
    at_start = jnp.logical_and(lax.axis_index("tm") == 0, lax.axis_index("grp") == 0)
    head_scale = jnp.where(at_start, 1.0, 0.0)

    def block(s, i, scale, shift, first):
        at = pl.multiple_of(i * SUB, SUB)
        new_scale, new_shift = [], []
        for j in range(groups):
            for k in range(SUB):
                lane = j * GROUP + k * LANES
                row = (j * SUB + k) * SUB
                gate_tmp[row : row + SUB, :] = gate_ref[s, pl.ds(at, SUB), lane : lane + LANES].astype(jnp.float32)
                cand_tmp[row : row + SUB, :] = cand_ref[s, pl.ds(at, SUB), lane : lane + LANES].astype(jnp.float32)
        for j in range(groups):
            mg = mg_ref[j]
            mc = mc_ref[j]
            a, b = scale[j], shift[j]
            for t in range(SUB):
                g = gate_tmp[pl.ds(j * SUB * SUB + t, SUB, stride=SUB), :]
                c = cand_tmp[pl.ds(j * SUB * SUB + t, SUB, stride=SUB), :]
                gate_rows_ref[s * groups + j, at + t] = g
                cand_rows_ref[s * groups + j, at + t] = c
                if first and t == 0:
                    sl, of = coefficients(g, c, start_ref[s * groups + j] * head_scale, mg, mc)
                    a, b = sl, of
                else:
                    sl, of = coefficients_at_zero(g, c, mg, mc)
                    a, b = sl * a, sl * b + of
                slopes_ref[s * groups + j, at + t] = sl
                offset_ref[s * groups + j, at + t] = of
            new_scale.append(a)
            new_shift.append(b)
        return tuple(new_scale), tuple(new_shift)

    for s in range(seqs):
        none = (None,) * groups
        carry = block(s, 0, none, none, True)
        scale, shift = lax.fori_loop(1, steps // SUB, lambda i, c: block(s, i, c[0], c[1], False), carry)
        for j in range(groups):
            map_ref[s * groups + j, :SUB] = scale[j]
            map_ref[s * groups + j, SUB:] = shift[j]


def next_kernel(seqs, steps, groups, gate_rows_ref, cand_rows_ref, old_slopes_ref, old_offset_ref, entry_ref,
                mg_ref, mc_ref, slopes_ref, offset_ref, map_ref):
    def block(s, i, state, scale, shift, first):
        at = pl.multiple_of(i * SUB, SUB)
        new_state, new_scale, new_shift = [], [], []
        for j in range(groups):
            n = s * groups + j
            mg = mg_ref[j]
            mc = mc_ref[j]
            e = state[j]
            a, b = scale[j], shift[j]
            for t in range(SUB):
                sl, of = coefficients(gate_rows_ref[n, at + t], cand_rows_ref[n, at + t], e, mg, mc)
                if first and t == 0:
                    a, b = sl, of
                else:
                    a, b = sl * a, sl * b + of
                slopes_ref[n, at + t] = sl
                offset_ref[n, at + t] = of
                e = old_slopes_ref[n, at + t] * e + old_offset_ref[n, at + t]
            new_state.append(e)
            new_scale.append(a)
            new_shift.append(b)
        return tuple(new_state), tuple(new_scale), tuple(new_shift)

    for s in range(seqs):
        none = (None,) * groups
        entry = tuple(entry_ref[s * groups + j] for j in range(groups))
        carry = block(s, 0, entry, none, none, True)
        _, scale, shift = lax.fori_loop(1, steps // SUB, lambda i, c: block(s, i, *c, False), carry)
        for j in range(groups):
            map_ref[s * groups + j, :SUB] = scale[j]
            map_ref[s * groups + j, SUB:] = shift[j]


def last_kernel(seqs, steps, groups, slopes_ref, offset_ref, entry_ref, out_ref, tmp):
    def block(s, i, state):
        at = pl.multiple_of(i * SUB, SUB)
        new_state = []
        for j in range(groups):
            n = s * groups + j
            e = state[j]
            for t in range(SUB):
                e = slopes_ref[n, at + t] * e + offset_ref[n, at + t]
                row = (j * SUB + t) * SUB
                tmp[row : row + SUB, :] = e
            new_state.append(e)
        for j in range(groups):
            for k in range(SUB):
                lane = j * GROUP + k * LANES
                rows = tmp[pl.ds(j * SUB * SUB + k, SUB, stride=SUB), :]
                out_ref[s, pl.ds(at, SUB), lane : lane + LANES] = rows.astype(jnp.bfloat16)
        return tuple(new_state)

    for s in range(seqs):
        entry = tuple(entry_ref[s * groups + j] for j in range(groups))
        lax.fori_loop(0, steps // SUB, lambda i, c: block(s, i, c), entry)


def compose_kernel(members, blocks, map_ref, out_ref):
    a, b = map_ref[0, :SUB], map_ref[0, SUB:]
    for z in range(1, members):
        sl = map_ref[z, :SUB]
        a, b = sl * a, sl * b + map_ref[z, SUB:]
    for d in range(blocks):
        out_ref[d, :SUB] = a
        out_ref[d, SUB:] = b


def entry_kernel(members, blocks, start_ref, block_maps_ref, map_ref, out_ref):
    me = lax.axis_index("tm")
    e = start_ref[lax.axis_index("grp")]
    for d in range(blocks):
        e = jnp.where(d < me, block_maps_ref[d, :SUB] * e + block_maps_ref[d, SUB:], e)
    for z in range(members):
        out_ref[z] = e
        if z < members - 1:
            e = map_ref[z, :SUB] * e + map_ref[z, SUB:]


def call(kernel, outs, scratch, *args):
    return pl.pallas_call(
        kernel,
        out_shape=outs,
        in_specs=[VMEM] * len(args),
        out_specs=jax.tree.map(lambda _: VMEM, outs),
        scratch_shapes=scratch,
        compiler_params=pltpu.CompilerParams(vmem_limit_bytes=24 * 2**20),
    )(*args)


def on_device(gate_pre, cand_pre, start_state, mix_gate, mix_cand):
    seqs, steps, width = gate_pre.shape
    groups = width // GROUP
    slabs = seqs * groups
    members, blocks = lax.axis_size("grp"), lax.axis_size("tm")
    f32 = functools.partial(jax.ShapeDtypeStruct, dtype=jnp.float32)
    start = start_state.reshape(slabs, SUB, LANES)
    mg = mix_gate.reshape(groups, SUB, LANES)
    mc = mix_cand.reshape(groups, SUB, LANES)
    rows = f32((slabs, steps, SUB, LANES))
    maps = f32((slabs, 2 * SUB, LANES))

    def entries(local_map):
        got = lax.all_to_all(local_map, "grp", 0, 0, tiled=True)
        sent = call(functools.partial(compose_kernel, members, blocks), f32((blocks, 2 * SUB, LANES)), [], got)
        block_maps = lax.all_to_all(sent, "tm", 0, 0, tiled=True)
        mine = call(functools.partial(entry_kernel, members, blocks), f32((members, SUB, LANES)), [],
                    start, block_maps, got)
        return lax.all_to_all(mine, "grp", 0, 0, tiled=True)

    tmp = pltpu.VMEM((groups * SUB * SUB, LANES), jnp.float32)
    slopes, offset, gate_rows, cand_rows, local = call(
        functools.partial(first_kernel, seqs, steps, groups), [rows, rows, rows, rows, maps], [tmp, tmp],
        gate_pre, cand_pre, start, mg, mc)
    entry = entries(local)
    for _ in range(2):
        slopes, offset, local = call(
            functools.partial(next_kernel, seqs, steps, groups), [rows, rows, maps], [],
            gate_rows, cand_rows, slopes, offset, entry, mg, mc)
        entry = entries(local)
    return call(
        functools.partial(last_kernel, seqs, steps, groups),
        jax.ShapeDtypeStruct(gate_pre.shape, jnp.bfloat16), [tmp], slopes, offset, entry)


def solution(mesh):
    in_specs = (P(None, ("tm", "grp"), None), P(None, ("tm", "grp"), None), P(), P(), P())
    out_specs = P(None, ("tm", "grp"), None)
    return jax.shard_map(
        on_device, mesh=mesh, in_specs=in_specs, out_specs=out_specs, check_vma=False
    )
```

```python
import functools

import jax
import jax.numpy as jnp
from jax import lax
from jax.experimental import pallas as pl
from jax.experimental.pallas import tpu as pltpu
from jax.sharding import Mesh
from jax.sharding import PartitionSpec as P

LANES = 128
SUB = 8
HALF = SUB // 2
GROUP = SUB * LANES
VMEM = pl.BlockSpec(memory_space=pltpu.VMEM)


def sigmoid(x):
    return 0.5 * jnp.tanh(0.5 * x) + 0.5


def coefficients(gate_in, cand_in, previous, mix_gate, mix_cand):
    forget = sigmoid(gate_in + mix_gate * previous)
    candidate = jnp.tanh(cand_in + mix_cand * previous)
    gap = previous - candidate
    kept = forget * gap
    slopes = forget + (1.0 - forget) * (kept * mix_gate + (mix_cand - candidate * candidate * mix_cand))
    offset = candidate + kept - slopes * previous
    return slopes, offset


def coefficients_at_zero(gate_in, cand_in, mix_gate, mix_cand):
    forget = sigmoid(gate_in)
    candidate = jnp.tanh(cand_in)
    kept = forget * candidate
    slopes = forget + (1.0 - forget) * ((mix_cand - candidate * candidate * mix_cand) - kept * mix_gate)
    return slopes, candidate - kept


def entry_row(entry_ref, n):
    return jnp.concatenate([entry_ref[2 * n], entry_ref[2 * n + 1]], axis=0)


def pieces(n, scale, shift, map_ref):
    for h in range(2):
        map_ref[2 * n + h, :HALF] = scale[h * HALF : (h + 1) * HALF]
        map_ref[2 * n + h, HALF:] = shift[h * HALF : (h + 1) * HALF]


def first_kernel(seqs, steps, groups, gate_ref, cand_ref, start_ref, mg_ref, mc_ref,
                 slopes_ref, offset_ref, gate_rows_ref, cand_rows_ref, map_ref, start_rows_ref, gate_tmp, cand_tmp):
    for s in range(seqs):
        for j in range(groups):
            for k in range(SUB):
                lane = j * GROUP + k * LANES
                start_rows_ref[s * groups + j, k : k + 1, :] = start_ref[s : s + 1, lane : lane + LANES]

    at_start = jnp.logical_and(
        jnp.logical_and(lax.axis_index("yx") == 0, lax.axis_index("c") == 0), lax.axis_index("grp") == 0)
    head_scale = jnp.where(at_start, 1.0, 0.0)

    def block(s, i, scale, shift, first):
        at = i * SUB if isinstance(i, int) else pl.multiple_of(i * SUB, SUB)
        new_scale, new_shift = [], []
        for j in range(groups):
            for k in range(SUB):
                lane = j * GROUP + k * LANES
                row = (j * SUB + k) * SUB
                gate_tmp[row : row + SUB, :] = gate_ref[s, pl.ds(at, SUB), lane : lane + LANES].astype(jnp.float32)
                cand_tmp[row : row + SUB, :] = cand_ref[s, pl.ds(at, SUB), lane : lane + LANES].astype(jnp.float32)
        for j in range(groups):
            mg = mg_ref[j]
            mc = mc_ref[j]
            a, b = scale[j], shift[j]
            for t in range(SUB):
                g = gate_tmp[pl.ds(j * SUB * SUB + t, SUB, stride=SUB), :]
                c = cand_tmp[pl.ds(j * SUB * SUB + t, SUB, stride=SUB), :]
                gate_rows_ref[s * groups + j, at + t] = g
                cand_rows_ref[s * groups + j, at + t] = c
                if first and t == 0:
                    sl, of = coefficients(g, c, start_rows_ref[s * groups + j] * head_scale, mg, mc)
                    a, b = sl, of
                else:
                    sl, of = coefficients_at_zero(g, c, mg, mc)
                    a, b = sl * a, sl * b + of
                slopes_ref[s * groups + j, at + t] = sl
                offset_ref[s * groups + j, at + t] = of
            new_scale.append(a)
            new_shift.append(b)
        return tuple(new_scale), tuple(new_shift)

    for s in range(seqs):
        none = (None,) * groups
        carry = block(s, 0, none, none, True)
        carry = lax.fori_loop(1, steps // SUB, lambda i, c: block(s, i, *c, False), carry)
        for j in range(groups):
            pieces(s * groups + j, carry[0][j], carry[1][j], map_ref)


def next_kernel(seqs, steps, groups, gate_rows_ref, cand_rows_ref, old_slopes_ref, old_offset_ref, entry_ref,
                mg_ref, mc_ref, slopes_ref, offset_ref, map_ref):
    def block(s, i, state, scale, shift, first):
        at = pl.multiple_of(i * SUB, SUB)
        new_state, new_scale, new_shift = [], [], []
        for j in range(groups):
            n = s * groups + j
            mg = mg_ref[j]
            mc = mc_ref[j]
            e = state[j]
            a, b = scale[j], shift[j]
            for t in range(SUB):
                sl, of = coefficients(gate_rows_ref[n, at + t], cand_rows_ref[n, at + t], e, mg, mc)
                if first and t == 0:
                    a, b = sl, of
                else:
                    a, b = sl * a, sl * b + of
                slopes_ref[n, at + t] = sl
                offset_ref[n, at + t] = of
                e = old_slopes_ref[n, at + t] * e + old_offset_ref[n, at + t]
            new_state.append(e)
            new_scale.append(a)
            new_shift.append(b)
        return tuple(new_state), tuple(new_scale), tuple(new_shift)

    for s in range(seqs):
        none = (None,) * groups
        entry = tuple(entry_row(entry_ref, s * groups + j) for j in range(groups))
        carry = block(s, 0, entry, none, none, True)
        _, scale, shift = lax.fori_loop(1, steps // SUB, lambda i, c: block(s, i, *c, False), carry)
        for j in range(groups):
            pieces(s * groups + j, scale[j], shift[j], map_ref)


def last_kernel(seqs, steps, groups, slopes_ref, offset_ref, entry_ref, out_ref, tmp):
    def block(s, i, state):
        at = pl.multiple_of(i * SUB, SUB)
        new_state = []
        for j in range(groups):
            n = s * groups + j
            e = state[j]
            for t in range(SUB):
                e = slopes_ref[n, at + t] * e + offset_ref[n, at + t]
                row = (j * SUB + t) * SUB
                tmp[row : row + SUB, :] = e
            new_state.append(e)
        for j in range(groups):
            for k in range(SUB):
                lane = j * GROUP + k * LANES
                rows = tmp[pl.ds(j * SUB * SUB + k, SUB, stride=SUB), :]
                out_ref[s, pl.ds(at, SUB), lane : lane + LANES] = rows.astype(jnp.bfloat16)
        return tuple(new_state)

    for s in range(seqs):
        entry = tuple(entry_row(entry_ref, s * groups + j) for j in range(groups))
        lax.fori_loop(0, steps // SUB, lambda i, c: block(s, i, c), entry)


def compose_kernel(members, blocks, map_ref, out_ref):
    a, b = map_ref[0, :HALF], map_ref[0, HALF:]
    for z in range(1, members):
        sl = map_ref[z, :HALF]
        a, b = sl * a, sl * b + map_ref[z, HALF:]
    for d in range(blocks):
        out_ref[d, :HALF] = a
        out_ref[d, HALF:] = b


def entry_kernel(members, blocks, start_ref, block_maps_ref, map_ref, out_ref):
    me = lax.axis_index("yx")
    c, z = lax.axis_index("c"), lax.axis_index("grp")
    piece = c * (members // 2) + z
    whole = start_ref[piece // 2]
    e = jnp.where(piece % 2 == 0, whole[:HALF], whole[HALF:])
    for d in range(blocks):
        e = jnp.where(d < me, block_maps_ref[d, :HALF] * e + block_maps_ref[d, HALF:], e)
    for m in range(members):
        out_ref[m] = e
        if m < members - 1:
            e = map_ref[m, :HALF] * e + map_ref[m, HALF:]


def call(kernel, outs, scratch, *args):
    return pl.pallas_call(
        kernel,
        out_shape=outs,
        in_specs=[VMEM] * len(args),
        out_specs=jax.tree.map(lambda _: VMEM, outs),
        scratch_shapes=scratch,
        compiler_params=pltpu.CompilerParams(vmem_limit_bytes=24 * 2**20),
    )(*args)


def on_device(gate_pre, cand_pre, start_state, mix_gate, mix_cand):
    seqs, steps, width = gate_pre.shape
    groups = width // GROUP
    slabs = seqs * groups
    members, blocks = lax.axis_size(("c", "grp")), lax.axis_size("yx")
    f32 = functools.partial(jax.ShapeDtypeStruct, dtype=jnp.float32)
    rows = f32((slabs, steps, SUB, LANES))
    maps = f32((2 * slabs, SUB, LANES))
    mix = (groups, SUB, LANES)

    tmp = pltpu.VMEM((groups * SUB * SUB, LANES), jnp.float32)
    mg, mc = mix_gate.reshape(mix), mix_cand.reshape(mix)
    slopes, offset, gate_rows, cand_rows, local, start = call(
        functools.partial(first_kernel, seqs, steps, groups),
        [rows, rows, rows, rows, maps, f32((slabs, SUB, LANES))], [tmp, tmp],
        gate_pre, cand_pre, start_state, mg, mc)

    def entries(local_map):
        got = lax.all_to_all(local_map, ("c", "grp"), 0, 0, tiled=True)
        sent = call(functools.partial(compose_kernel, members, blocks), f32((blocks, SUB, LANES)), [], got)
        block_maps = lax.all_to_all(sent, "yx", 0, 0, tiled=True)
        mine = call(functools.partial(entry_kernel, members, blocks), f32((members, HALF, LANES)), [],
                    start, block_maps, got)
        return lax.all_to_all(mine, ("c", "grp"), 0, 0, tiled=True)

    entry = entries(local)
    for _ in range(2):
        slopes, offset, local = call(
            functools.partial(next_kernel, seqs, steps, groups), [rows, rows, maps], [],
            gate_rows, cand_rows, slopes, offset, entry, mg, mc)
        entry = entries(local)
    return call(
        functools.partial(last_kernel, seqs, steps, groups),
        jax.ShapeDtypeStruct(gate_pre.shape, jnp.bfloat16), [tmp], slopes, offset, entry)


def solution(mesh):
    tm, grp = mesh.shape["tm"], mesh.shape["grp"]
    finer = Mesh(mesh.devices.reshape(tm // 2, 2, grp), ("yx", "c", "grp"))
    time = P(None, ("yx", "c", "grp"), None)
    return jax.shard_map(
        on_device, mesh=finer, in_specs=(time, time, P(), P(), P()), out_specs=time, check_vma=False
    )
```

```python
import functools

import jax
import jax.numpy as jnp
from jax import lax
from jax.experimental import pallas as pl
from jax.experimental.pallas import tpu as pltpu
from jax.sharding import PartitionSpec as P

LANES = 128
SUB = 8
PARTS = 4
WIDE = LANES // PARTS
GROUP = SUB * LANES
VMEM = pl.BlockSpec(memory_space=pltpu.VMEM)


def sigmoid(x):
    return 0.5 * jnp.tanh(0.5 * x) + 0.5


def coefficients(gate_in, cand_in, previous, mix_gate, mix_cand):
    forget = sigmoid(gate_in + mix_gate * previous)
    candidate = jnp.tanh(cand_in + mix_cand * previous)
    gap = previous - candidate
    kept = forget * gap
    slopes = forget + (1.0 - forget) * (kept * mix_gate + (mix_cand - candidate * candidate * mix_cand))
    offset = candidate + kept - slopes * previous
    return slopes, offset


def coefficients_at_zero(gate_in, cand_in, mix_gate, mix_cand):
    forget = sigmoid(gate_in)
    candidate = jnp.tanh(cand_in)
    kept = forget * candidate
    slopes = forget + (1.0 - forget) * ((mix_cand - candidate * candidate * mix_cand) - kept * mix_gate)
    return slopes, candidate - kept


def lane_part():
    return lax.broadcasted_iota(jnp.int32, (SUB, LANES), 1) // WIDE


def roll_parts(x, parts):
    parts %= PARTS
    return pltpu.roll(x, parts * WIDE, 1) if parts else x


def swap_parts(rows, part):
    low = part < 2
    even = part % 2 == 0
    half = [
        [jnp.where(low, rows[u], roll_parts(rows[u + 2], 2)) for u in range(2)],
        [jnp.where(low, roll_parts(rows[u], 2), rows[u + 2]) for u in range(2)],
    ]
    done = []
    for a, b in half:
        done.append(jnp.where(even, a, roll_parts(b, 1)))
        done.append(jnp.where(even, roll_parts(a, 3), b))
    return done


def pack_kernel(seqs, steps, groups, gate_ref, cand_ref, out_ref, *tmp):
    part = lane_part()
    rows = steps // PARTS
    owners = PARTS * SUB

    def slab(n, _):
        s = n // groups
        base = (n % groups) * GROUP
        for half, (in_ref, flat) in enumerate(zip((gate_ref, cand_ref), tmp[:2], strict=True)):
            for k in range(SUB):
                for i in range(steps // SUB):
                    lane = pl.multiple_of(base + k * LANES, LANES)
                    at = k * steps + i * SUB
                    flat[at : at + SUB, :] = in_ref[s, i * SUB : (i + 1) * SUB, pl.ds(lane, LANES)].astype(jnp.float32)
            for r in range(rows):
                got = [flat[pl.ds(u * rows + r, SUB, stride=steps), :] for u in range(PARTS)]
                for q, row in enumerate(swap_parts(got, part)):
                    at = q * SUB * 2 * rows + half * rows + r
                    tmp[2][pl.ds(at, SUB, stride=2 * rows), :] = row
        for d in range(owners):
            out_ref[n * owners + d] = tmp[2][d * 2 * rows : (d + 1) * 2 * rows, :].astype(jnp.bfloat16)
        return 0

    lax.fori_loop(0, seqs * groups, slab, 0)


def repeat_first_part(x, part):
    x = jnp.where(part == 0, x, roll_parts(x, 1))
    return jnp.where(part < 2, x, roll_parts(x, 2))


def repeat_last_part(x, part):
    x = jnp.where(part == 3, x, roll_parts(x, 3))
    return jnp.where(part >= 2, x, roll_parts(x, 2))


def own_row(ref, n, k, q, part):
    row = jnp.broadcast_to(ref[n, pl.ds(k, 1), :], (SUB, LANES))
    return repeat_first_part(pltpu.roll(row, ((PARTS - q) % PARTS) * WIDE, 1), part)


def owner_kernel(groups, tiles, rows, got_ref, start_ref, mg_all_ref, mc_all_ref, out_ref,
                 flat, slopes_ref, offset_ref, scale_ref, shift_ref, entry_ref):
    part = lane_part()
    sub = lax.broadcasted_iota(jnp.int32, (SUB, LANES), 0)
    owner = lax.axis_index("tm") * lax.axis_size("grp") + lax.axis_index("grp")
    n, q, k = owner // (PARTS * SUB), (owner // SUB) % PARTS, owner % SUB
    mg = own_row(mg_all_ref, n % groups, k, q, part)
    mc = own_row(mc_all_ref, n % groups, k, q, part)
    start = own_row(start_ref, n, k, q, part)
    per = 2 * rows * SUB

    def unpack(v, _):
        at = pl.multiple_of(v * per, per)
        for m in range(SUB):
            flat[pl.ds(at + m * 2 * rows, 2 * rows), :] = got_ref[v * SUB + m].astype(jnp.float32)
        return 0

    def inputs(v, r):
        return (flat[pl.ds(v * per + r, SUB, stride=2 * rows), :],
                flat[pl.ds(v * per + rows + r, SUB, stride=2 * rows), :])

    def first(v, _):
        head = jnp.where(jnp.logical_and(v == 0, jnp.logical_and(sub == 0, part == 0)), start, 0.0)
        for r in range(rows):
            g, c = inputs(v, r)
            if r == 0:
                sl, of = coefficients(g, c, head, mg, mc)
                a, b = sl, of
            else:
                sl, of = coefficients_at_zero(g, c, mg, mc)
                a, b = sl * a, sl * b + of
            slopes_ref[v, r] = sl
            offset_ref[v, r] = of
        scale_ref[v] = a
        shift_ref[v] = b
        return 0

    def following(last, v, _):
        e = entry_ref[v]
        for r in range(rows):
            sl, of = coefficients(*inputs(v, r), e, mg, mc)
            a, b = (sl, of) if r == 0 else (sl * a, sl * b + of)
            if r < rows - 1:
                e = slopes_ref[v, r] * e + offset_ref[v, r]
            if not last:
                slopes_ref[v, r] = sl
                offset_ref[v, r] = of
        scale_ref[v] = a
        shift_ref[v] = b
        return 0

    def scan(v, state):
        a, b = scale_ref[v], shift_ref[v]
        for step in (1, 2):
            earlier_a = jnp.where(part >= step, roll_parts(a, step), 1.0)
            earlier_b = jnp.where(part >= step, roll_parts(b, step), 0.0)
            a, b = a * earlier_a, a * earlier_b + b
        part_a = jnp.where(part >= 1, roll_parts(a, 1), 1.0)
        part_b = jnp.where(part >= 1, roll_parts(b, 1), 0.0)
        a, b = repeat_last_part(a, part), repeat_last_part(b, part)
        for step in (1, 2, 4):
            earlier_a = jnp.where(sub >= step, pltpu.roll(a, step, 0), 1.0)
            earlier_b = jnp.where(sub >= step, pltpu.roll(b, step, 0), 0.0)
            a, b = a * earlier_a, a * earlier_b + b
        sub_a = jnp.where(sub >= 1, pltpu.roll(a, 1, 0), 1.0)
        sub_b = jnp.where(sub >= 1, pltpu.roll(b, 1, 0), 0.0)
        entry_ref[v] = part_a * (sub_a * state + sub_b) + part_b
        whole_a = jnp.broadcast_to(a[SUB - 1 : SUB], (SUB, LANES))
        whole_b = jnp.broadcast_to(b[SUB - 1 : SUB], (SUB, LANES))
        return whole_a * state + whole_b

    def entries(i):
        lax.fori_loop(0, tiles, scan, start, unroll=4)
        for v in range(tiles):
            at = v * SUB
            moved = roll_parts(entry_ref[v], i)
            out_ref[at : at + SUB, :] = moved if i == 0 else jnp.where(part == i, moved, out_ref[at : at + SUB, :])

    lax.fori_loop(0, tiles, unpack, 0)
    lax.fori_loop(0, tiles, first, 0, unroll=2)
    entries(0)
    lax.fori_loop(0, tiles, functools.partial(following, False), 0, unroll=2)
    entries(1)
    lax.fori_loop(0, tiles, functools.partial(following, True), 0, unroll=2)
    entries(2)


def last_kernel(seqs, steps, groups, gate_ref, cand_ref, entry_ref, mg_ref, mc_ref, out_ref, gate_tmp, cand_tmp):
    part = lane_part()
    at_start = jnp.logical_and(lax.axis_index("tm") == 0, lax.axis_index("grp") == 0)
    head_scale = jnp.where(at_start, 1.0, 0.0)

    def entry_rows(n):
        got = [entry_ref[(n * PARTS + q) * SUB : (n * PARTS + q + 1) * SUB, :] for q in range(PARTS)]
        rows = []
        for i in range(3):
            row = roll_parts(got[0], -i)
            for q in range(1, PARTS):
                row = jnp.where(part == q, roll_parts(got[q], q - i), row)
            rows.append(row)
        return tuple(rows)

    def block(s, i, states, begin):
        at = i * SUB if isinstance(i, int) else pl.multiple_of(i * SUB, SUB)
        done = []
        for j in range(groups):
            for k in range(SUB):
                lane = j * GROUP + k * LANES
                row = (j * SUB + k) * SUB
                gate_tmp[row : row + SUB, :] = gate_ref[s, pl.ds(at, SUB), lane : lane + LANES].astype(jnp.float32)
                cand_tmp[row : row + SUB, :] = cand_ref[s, pl.ds(at, SUB), lane : lane + LANES].astype(jnp.float32)
        for j in range(groups):
            mg, mc = mg_ref[j], mc_ref[j]
            first, second, third = states[j]
            for t in range(SUB):
                window = pl.ds(j * SUB * SUB + t, SUB, stride=SUB)
                g, c = gate_tmp[window, :], cand_tmp[window, :]
                if begin and t == 0:
                    sl1, of1 = coefficients(g, c, first * head_scale, mg, mc)
                else:
                    sl1, of1 = coefficients_at_zero(g, c, mg, mc)
                sl2, of2 = coefficients(g, c, first, mg, mc)
                sl3, of3 = coefficients(g, c, second, mg, mc)
                first = sl1 * first + of1
                second = sl2 * second + of2
                third = sl3 * third + of3
                gate_tmp[window, :] = third
            done.append((first, second, third))
            for k in range(SUB):
                lane = j * GROUP + k * LANES
                row = (j * SUB + k) * SUB
                out_ref[s, pl.ds(at, SUB), lane : lane + LANES] = gate_tmp[row : row + SUB, :].astype(jnp.bfloat16)
        return tuple(done)

    for s in range(seqs):
        states = tuple(entry_rows(s * groups + j) for j in range(groups))
        states = block(s, 0, states, True)
        lax.fori_loop(1, steps // SUB, lambda i, c: block(s, i, c, False), states)


def call(kernel, outs, scratch, *args):
    return pl.pallas_call(
        kernel,
        out_shape=outs,
        in_specs=[VMEM] * len(args),
        out_specs=jax.tree.map(lambda _: VMEM, outs),
        scratch_shapes=scratch,
        compiler_params=pltpu.CompilerParams(vmem_limit_bytes=32 * 2**20),
    )(*args)


def on_device(gate_pre, cand_pre, start_state, mix_gate, mix_cand):
    seqs, steps, width = gate_pre.shape
    groups = width // GROUP
    slabs = seqs * groups
    axes = ("tm", "grp")
    owners = lax.axis_size(axes)
    rows = steps // PARTS
    tiles = owners // SUB
    f32 = functools.partial(jax.ShapeDtypeStruct, dtype=jnp.float32)

    def scratch(*shape):
        return pltpu.VMEM(shape, jnp.float32)

    mg = mix_gate.reshape(groups, SUB, LANES)
    mc = mix_cand.reshape(groups, SUB, LANES)
    start = start_state.reshape(slabs, SUB, LANES)
    packed = call(
        functools.partial(pack_kernel, seqs, steps, groups),
        jax.ShapeDtypeStruct((owners, 2 * rows, LANES), jnp.bfloat16),
        [scratch(SUB * steps, LANES), scratch(SUB * steps, LANES), scratch(PARTS * SUB * 2 * rows, LANES)],
        gate_pre, cand_pre)
    got = lax.all_to_all(packed, axes, 0, 0, tiled=True)
    states = call(
        functools.partial(owner_kernel, groups, tiles, rows), f32((owners, LANES)),
        [scratch(owners * 2 * rows, LANES), scratch(tiles, rows, SUB, LANES), scratch(tiles, rows, SUB, LANES),
         scratch(tiles, SUB, LANES), scratch(tiles, SUB, LANES), scratch(tiles, SUB, LANES)],
        got, start, mg, mc)
    entry = lax.all_to_all(states.reshape(owners, 1, LANES), axes, 0, 0, tiled=True).reshape(owners, LANES)
    tmp = scratch(groups * SUB * SUB, LANES)
    return call(
        functools.partial(last_kernel, seqs, steps, groups),
        jax.ShapeDtypeStruct(gate_pre.shape, jnp.bfloat16), [tmp, tmp], gate_pre, cand_pre, entry, mg, mc)


def solution(mesh):
    time = P(None, ("tm", "grp"), None)
    return jax.shard_map(
        on_device, mesh=mesh, in_specs=(time, time, P(), P(), P()), out_specs=time, check_vma=False
    )
```

```python
import functools

import jax
import jax.numpy as jnp
from jax import lax
from jax.experimental import pallas as pl
from jax.experimental.pallas import tpu as pltpu
from jax.sharding import PartitionSpec as P

LANES = 128
SUB = 8
PARTS = 4
WIDE = LANES // PARTS
GROUP = SUB * LANES
PAD = SUB


def forget_and_rest(half_gate):
    half = 0.5 * jnp.tanh(half_gate)
    return 0.5 + half, 0.5 - half


def coefficients(half_gate, cand_in, previous, half_mix_gate, mix_gate, mix_cand):
    forget, rest = forget_and_rest(half_gate + half_mix_gate * previous)
    candidate = jnp.tanh(cand_in + mix_cand * previous)
    kept = forget * (previous - candidate)
    slopes = forget + rest * (kept * mix_gate + (mix_cand - candidate * candidate * mix_cand))
    return slopes, candidate + kept


def coefficients_at_zero(half_gate, cand_in, mix_gate, mix_cand):
    forget, rest = forget_and_rest(half_gate)
    candidate = jnp.tanh(cand_in)
    kept = forget * candidate
    slopes = forget + rest * ((mix_cand - candidate * candidate * mix_cand) - kept * mix_gate)
    return slopes, candidate - kept


def lane_part():
    return lax.broadcasted_iota(jnp.int32, (SUB, LANES), 1) // WIDE


def roll_parts(x, parts):
    parts %= PARTS
    return pltpu.roll(x, parts * WIDE, 1) if parts else x


def swap_parts(rows, part):
    low = part < 2
    even = part % 2 == 0
    half = [
        [jnp.where(low, rows[u], roll_parts(rows[u + 2], 2)) for u in range(2)],
        [jnp.where(low, roll_parts(rows[u], 2), rows[u + 2]) for u in range(2)],
    ]
    done = []
    for a, b in half:
        done.append(jnp.where(even, a, roll_parts(b, 1)))
        done.append(jnp.where(even, roll_parts(a, 3), b))
    return done


def pack_kernel(seqs, steps, groups, gate_hbm, cand_hbm, out_hbm,
                gate_ref, cand_ref, packed, gate_flat, cand_flat, mixed, in_sem, out_sem):
    part = lane_part()
    rows = steps // PARTS
    owners = PARTS * SUB
    slabs = seqs * groups
    stride = steps + PAD
    piece = 2 * rows + PAD

    def fetch(n):
        s, lane = n // groups, pl.multiple_of((n % groups) * GROUP, GROUP)
        window = (s, slice(None), pl.ds(lane, GROUP))
        return [
            pltpu.make_async_copy(gate_hbm.at[window], gate_ref.at[n], in_sem.at[0, n]),
            pltpu.make_async_copy(cand_hbm.at[window], cand_ref.at[n], in_sem.at[1, n]),
        ]

    def store(n):
        at = pl.multiple_of(n * owners, owners)
        return pltpu.make_async_copy(packed.at[pl.ds(at, owners)], out_hbm.at[pl.ds(at, owners)], out_sem.at[n])

    for n in range(slabs):
        for copy in fetch(n):
            copy.start()

    def slab(n, _):
        for copy in fetch(n):
            copy.wait()
        for half, (in_ref, flat) in enumerate(((gate_ref, gate_flat), (cand_ref, cand_flat))):
            for k in range(SUB):
                for i in range(steps // SUB):
                    at = k * stride + i * SUB
                    flat[at : at + SUB, :] = in_ref[
                        n, i * SUB : (i + 1) * SUB, k * LANES : (k + 1) * LANES].astype(jnp.float32)
            for r in range(rows):
                got = [flat[pl.ds(u * rows + r, SUB, stride=stride), :] for u in range(PARTS)]
                for q, row in enumerate(swap_parts(got, part)):
                    mixed[pl.ds(q * SUB * piece + half * rows + r, SUB, stride=piece), :] = row
        for d in range(owners):
            packed[n * owners + d] = mixed[d * piece : d * piece + 2 * rows, :].astype(jnp.bfloat16)
        store(n).start()
        return 0

    lax.fori_loop(0, slabs, slab, 0)
    for n in range(slabs):
        store(n).wait()


def repeat_first_part(x, part):
    x = jnp.where(part == 0, x, roll_parts(x, 1))
    return jnp.where(part < 2, x, roll_parts(x, 2))


def repeat_last_part(x, part):
    x = jnp.where(part == 3, x, roll_parts(x, 3))
    return jnp.where(part >= 2, x, roll_parts(x, 2))


def own_row(ref, n, k, q, part):
    row = jnp.broadcast_to(ref[n, pl.ds(k, 1), :], (SUB, LANES))
    return repeat_first_part(pltpu.roll(row, ((PARTS - q) % PARTS) * WIDE, 1), part)


def owner_kernel(groups, tiles, rows, got_ref, start_ref, mg_all_ref, mc_all_ref, out_ref,
                 flat, slopes_ref, offset_ref, scale_ref, shift_ref, entry_ref):
    part = lane_part()
    sub = lax.broadcasted_iota(jnp.int32, (SUB, LANES), 0)
    owner = lax.axis_index("tm") * lax.axis_size("grp") + lax.axis_index("grp")
    n, q, k = owner // (PARTS * SUB), (owner // SUB) % PARTS, owner % SUB
    mg = own_row(mg_all_ref, n % groups, k, q, part)
    half_mg = 0.5 * mg
    mc = own_row(mc_all_ref, n % groups, k, q, part)
    start = own_row(start_ref, n, k, q, part)
    piece = 2 * rows + PAD
    per = piece * SUB

    def unpack(v, _):
        at = pl.multiple_of(v * per, SUB)
        for m in range(SUB):
            got = got_ref[v * SUB + m].astype(jnp.float32)
            flat[pl.ds(at + m * piece, rows), :] = 0.5 * got[:rows]
            flat[pl.ds(at + m * piece + rows, rows), :] = got[rows:]
        return 0

    def inputs(v, r):
        return (flat[pl.ds(v * per + r, SUB, stride=piece), :],
                flat[pl.ds(v * per + rows + r, SUB, stride=piece), :])

    def first(v, _):
        head = jnp.where(jnp.logical_and(v == 0, jnp.logical_and(sub == 0, part == 0)), start, 0.0)
        for r in range(rows):
            g, c = inputs(v, r)
            if r == 0:
                sl, of = coefficients(g, c, head, half_mg, mg, mc)
                of -= sl * head
                a, b = sl, of
            else:
                sl, of = coefficients_at_zero(g, c, mg, mc)
                a, b = sl * a, sl * b + of
            slopes_ref[v, r] = sl
            offset_ref[v, r] = of
        scale_ref[v] = a
        shift_ref[v] = b
        return 0

    def following(last, v, _):
        e = entry_ref[v]
        for r in range(rows):
            sl, at_slope = coefficients(*inputs(v, r), e, half_mg, mg, mc)
            if last:
                a, b = (sl, at_slope - sl * e) if r == 0 else (sl * a, sl * (b - e) + at_slope)
            else:
                of = at_slope - sl * e
                a, b = (sl, of) if r == 0 else (sl * a, sl * b + of)
            if r < rows - 1:
                e = slopes_ref[v, r] * e + offset_ref[v, r]
            if not last:
                slopes_ref[v, r] = sl
                offset_ref[v, r] = of
        scale_ref[v] = a
        shift_ref[v] = b
        return 0

    def scan(v, state):
        a, b = scale_ref[v], shift_ref[v]
        for step in (1, 2):
            earlier_a = jnp.where(part >= step, roll_parts(a, step), 1.0)
            earlier_b = jnp.where(part >= step, roll_parts(b, step), 0.0)
            a, b = a * earlier_a, a * earlier_b + b
        part_a = jnp.where(part >= 1, roll_parts(a, 1), 1.0)
        part_b = jnp.where(part >= 1, roll_parts(b, 1), 0.0)
        a, b = repeat_last_part(a, part), repeat_last_part(b, part)
        for step in (1, 2, 4):
            earlier_a = jnp.where(sub >= step, pltpu.roll(a, step, 0), 1.0)
            earlier_b = jnp.where(sub >= step, pltpu.roll(b, step, 0), 0.0)
            a, b = a * earlier_a, a * earlier_b + b
        sub_a = jnp.where(sub >= 1, pltpu.roll(a, 1, 0), 1.0)
        sub_b = jnp.where(sub >= 1, pltpu.roll(b, 1, 0), 0.0)
        entry_ref[v] = part_a * (sub_a * state + sub_b) + part_b
        whole_a = jnp.broadcast_to(a[SUB - 1 : SUB], (SUB, LANES))
        whole_b = jnp.broadcast_to(b[SUB - 1 : SUB], (SUB, LANES))
        return whole_a * state + whole_b

    def entries(i):
        lax.fori_loop(0, tiles, scan, start, unroll=4)
        for v in range(tiles):
            at = v * SUB
            moved = roll_parts(entry_ref[v], i)
            out_ref[at : at + SUB, :] = moved if i == 0 else jnp.where(part == i, moved, out_ref[at : at + SUB, :])

    lax.fori_loop(0, tiles, unpack, 0)
    lax.fori_loop(0, tiles, first, 0, unroll=2)
    entries(0)
    lax.fori_loop(0, tiles, functools.partial(following, False), 0, unroll=2)
    entries(1)
    lax.fori_loop(0, tiles, functools.partial(following, True), 0, unroll=2)
    entries(2)


def last_kernel(seqs, steps, groups, gate_ref, cand_ref, entry_ref, mg_ref, mc_ref, out_ref,
                gate_tmp, cand_tmp, out_tmp):
    part = lane_part()
    at_start = jnp.logical_and(lax.axis_index("tm") == 0, lax.axis_index("grp") == 0)
    head_scale = jnp.where(at_start, 1.0, 0.0)

    def entry_rows(n):
        got = [entry_ref[(n * PARTS + q) * SUB : (n * PARTS + q + 1) * SUB, :] for q in range(PARTS)]
        rows = []
        for i in range(3):
            row = roll_parts(got[0], -i)
            for q in range(1, PARTS):
                row = jnp.where(part == q, roll_parts(got[q], q - i), row)
            rows.append(row)
        return tuple(rows)

    def block(s, i, states, begin):
        at = i * SUB if isinstance(i, int) else pl.multiple_of(i * SUB, SUB)
        done = []
        for j in range(groups):
            for k in range(SUB):
                lane = j * GROUP + k * LANES
                row = (j * SUB + k) * SUB
                gate = gate_ref[s, pl.ds(at, SUB), lane : lane + LANES].astype(jnp.float32)
                gate_tmp[row : row + SUB, :] = 0.5 * gate
                cand_tmp[row : row + SUB, :] = cand_ref[s, pl.ds(at, SUB), lane : lane + LANES].astype(jnp.float32)
        for j in range(groups):
            mg, mc = mg_ref[j], mc_ref[j]
            half_mg = 0.5 * mg
            first, second, third = states[j]
            for t in range(SUB):
                window = pl.ds(j * SUB * SUB + t, SUB, stride=SUB)
                g, c = gate_tmp[window, :], cand_tmp[window, :]
                sl2, at2 = coefficients(g, c, first, half_mg, mg, mc)
                sl3, at3 = coefficients(g, c, second, half_mg, mg, mc)
                third = sl3 * (third - second) + at3
                second = sl2 * (second - first) + at2
                if begin and t == 0:
                    head = first * head_scale
                    sl1, at1 = coefficients(g, c, head, half_mg, mg, mc)
                    first = sl1 * (first - head) + at1
                else:
                    sl1, at1 = coefficients_at_zero(g, c, mg, mc)
                    first = sl1 * first + at1
                row = (j * SUB + t) * SUB
                out_tmp[row : row + SUB, :] = third
            done.append((first, second, third))
            for k in range(SUB):
                lane = j * GROUP + k * LANES
                rows = out_tmp[pl.ds(j * SUB * SUB + k, SUB, stride=SUB), :]
                out_ref[s, pl.ds(at, SUB), lane : lane + LANES] = rows.astype(jnp.bfloat16)
        return tuple(done)

    for s in range(seqs):
        states = tuple(entry_rows(s * groups + j) for j in range(groups))
        states = block(s, 0, states, True)
        lax.fori_loop(1, steps // SUB, lambda i, c: block(s, i, c, False), states)


def call(kernel, outs, scratch, *args, vmem=32, space=pltpu.VMEM):
    spec = pl.BlockSpec(memory_space=space)
    return pl.pallas_call(
        kernel,
        out_shape=outs,
        in_specs=[spec] * len(args),
        out_specs=jax.tree.map(lambda _: spec, outs),
        scratch_shapes=scratch,
        compiler_params=pltpu.CompilerParams(vmem_limit_bytes=vmem * 2**20),
    )(*args)


def on_device(gate_pre, cand_pre, start_state, mix_gate, mix_cand):
    seqs, steps, width = gate_pre.shape
    groups = width // GROUP
    slabs = seqs * groups
    axes = ("tm", "grp")
    owners = lax.axis_size(axes)
    rows = steps // PARTS
    tiles = owners // SUB
    f32 = functools.partial(jax.ShapeDtypeStruct, dtype=jnp.float32)

    def scratch(*shape):
        return pltpu.VMEM(shape, jnp.float32)

    mg = mix_gate.reshape(groups, SUB, LANES)
    mc = mix_cand.reshape(groups, SUB, LANES)
    packed = call(
        functools.partial(pack_kernel, seqs, steps, groups),
        jax.ShapeDtypeStruct((owners, 2 * rows, LANES), jnp.bfloat16),
        [pltpu.VMEM((slabs, steps, GROUP), jnp.bfloat16), pltpu.VMEM((slabs, steps, GROUP), jnp.bfloat16),
         pltpu.VMEM((owners, 2 * rows, LANES), jnp.bfloat16),
         scratch(SUB * (steps + PAD), LANES), scratch(SUB * (steps + PAD), LANES),
         scratch(PARTS * SUB * (2 * rows + PAD), LANES),
         pltpu.SemaphoreType.DMA((2, slabs)), pltpu.SemaphoreType.DMA((slabs,))],
        gate_pre, cand_pre, vmem=56, space=pltpu.HBM)
    start = start_state.reshape(slabs, SUB, LANES)
    got = lax.all_to_all(packed, axes, 0, 0, tiled=True)
    tmp = scratch(groups * SUB * SUB, LANES)
    states = call(
        functools.partial(owner_kernel, groups, tiles, rows), f32((owners, LANES)),
        [scratch(owners * (2 * rows + PAD), LANES), scratch(tiles, rows, SUB, LANES), scratch(tiles, rows, SUB, LANES),
         scratch(tiles, SUB, LANES), scratch(tiles, SUB, LANES), scratch(tiles, SUB, LANES)],
        got, start, mg, mc, vmem=16)
    entry = lax.all_to_all(states.reshape(owners, 1, LANES), axes, 0, 0, tiled=True).reshape(owners, LANES)
    return call(
        functools.partial(last_kernel, seqs, steps, groups),
        jax.ShapeDtypeStruct(gate_pre.shape, jnp.bfloat16), [tmp, tmp, tmp],
        gate_pre, cand_pre, entry, mg, mc, vmem=16)


def solution(mesh):
    time = P(None, ("tm", "grp"), None)
    return jax.shard_map(
        on_device, mesh=mesh, in_specs=(time, time, P(), P(), P()), out_specs=time, check_vma=False
    )
```

```python
import functools

import jax
import jax.numpy as jnp
from jax import lax
from jax.experimental import pallas as pl
from jax.experimental.pallas import tpu as pltpu
from jax.sharding import PartitionSpec as P

LANES = 128
SUB = 8
PARTS = 4
WIDE = LANES // PARTS
GROUP = SUB * LANES


def forget_and_rest(half_gate):
    half = 0.5 * jnp.tanh(half_gate)
    return 0.5 + half, 0.5 - half


def coefficients(half_gate, cand_in, previous, half_mix_gate, mix_gate, mix_cand):
    forget, rest = forget_and_rest(half_gate + half_mix_gate * previous)
    candidate = jnp.tanh(cand_in + mix_cand * previous)
    kept = forget * (previous - candidate)
    slopes = forget + rest * (kept * mix_gate + (mix_cand - candidate * candidate * mix_cand))
    return slopes, candidate + kept


def coefficients_at_zero(half_gate, cand_in, mix_gate, mix_cand):
    forget, rest = forget_and_rest(half_gate)
    candidate = jnp.tanh(cand_in)
    kept = forget * candidate
    slopes = forget + rest * ((mix_cand - candidate * candidate * mix_cand) - kept * mix_gate)
    return slopes, candidate - kept


def lane_part():
    return lax.broadcasted_iota(jnp.int32, (SUB, LANES), 1) // WIDE


def roll_parts(x, parts):
    parts %= PARTS
    return pltpu.roll(x, parts * WIDE, 1) if parts else x


def swap_parts(rows, part):
    low = part < 2
    even = part % 2 == 0
    half = [
        [jnp.where(low, rows[u], roll_parts(rows[u + 2], 2)) for u in range(2)],
        [jnp.where(low, roll_parts(rows[u], 2), rows[u + 2]) for u in range(2)],
    ]
    done = []
    for a, b in half:
        done.append(jnp.where(even, a, roll_parts(b, 1)))
        done.append(jnp.where(even, roll_parts(a, 3), b))
    return done


def pack_kernel(seqs, steps, groups, gate_hbm, cand_hbm, out_hbm,
                gate_ref, cand_ref, packed, gate_flat, cand_flat, mixed, in_sem, out_sem):
    part = lane_part()
    rows = steps // PARTS
    owners = PARTS * SUB
    slabs = seqs * groups

    def fetch(n):
        s, lane = n // groups, pl.multiple_of((n % groups) * GROUP, GROUP)
        window = (s, slice(None), pl.ds(lane, GROUP))
        return [
            pltpu.make_async_copy(gate_hbm.at[window], gate_ref.at[n], in_sem.at[0, n]),
            pltpu.make_async_copy(cand_hbm.at[window], cand_ref.at[n], in_sem.at[1, n]),
        ]

    def store(n):
        at = pl.multiple_of(n * owners, owners)
        return pltpu.make_async_copy(packed.at[pl.ds(at, owners)], out_hbm.at[pl.ds(at, owners)], out_sem.at[n])

    for n in range(slabs):
        for copy in fetch(n):
            copy.start()

    def slab(n, _):
        for copy in fetch(n):
            copy.wait()
        for half, (in_ref, flat) in enumerate(((gate_ref, gate_flat), (cand_ref, cand_flat))):
            for i in range(steps // SUB):
                for k in range(SUB):
                    at = (i * SUB + k) * SUB
                    flat[at : at + SUB, :] = in_ref[
                        n, i * SUB : (i + 1) * SUB, k * LANES : (k + 1) * LANES].astype(jnp.float32)
            for r in range(rows):
                got = []
                for u in range(PARTS):
                    t = u * rows + r
                    got.append(flat[pl.ds(t // SUB * SUB * SUB + t % SUB, SUB, stride=SUB), :])
                for q, row in enumerate(swap_parts(got, part)):
                    at = (q * 2 * rows + half * rows + r) * SUB
                    mixed[at : at + SUB, :] = row
        for q in range(PARTS):
            for k in range(SUB):
                for g in range(rows // SUB):
                    at = (q * 2 * rows + g * 2 * SUB) * SUB + k
                    two = [mixed[pl.ds(at + h * SUB * SUB, SUB, stride=SUB), :] for h in range(2)]
                    packed[n * owners + q * SUB + k, g * 2 * SUB : (g + 1) * 2 * SUB, :] = jnp.concatenate(
                        two, axis=0).astype(jnp.bfloat16)
        store(n).start()
        return 0

    lax.fori_loop(0, slabs, slab, 0)
    for n in range(slabs):
        store(n).wait()


def repeat_first_part(x, part):
    x = jnp.where(part == 0, x, roll_parts(x, 1))
    return jnp.where(part < 2, x, roll_parts(x, 2))


def repeat_last_part(x, part):
    x = jnp.where(part == 3, x, roll_parts(x, 3))
    return jnp.where(part >= 2, x, roll_parts(x, 2))


def own_row(ref, n, k, q, part):
    row = jnp.broadcast_to(ref[n, pl.ds(k, 1), :], (SUB, LANES))
    return repeat_first_part(pltpu.roll(row, ((PARTS - q) % PARTS) * WIDE, 1), part)


def owner_kernel(groups, tiles, rows, got_ref, start_ref, mg_all_ref, mc_all_ref, out_ref,
                 flat, gate_ref, cand_ref, slopes_ref, offset_ref, scale_ref, shift_ref, entry_ref):
    part = lane_part()
    sub = lax.broadcasted_iota(jnp.int32, (SUB, LANES), 0)
    owner = lax.axis_index("tm") * lax.axis_size("grp") + lax.axis_index("grp")
    n, q, k = owner // (PARTS * SUB), (owner // SUB) % PARTS, owner % SUB
    mg = own_row(mg_all_ref, n % groups, k, q, part)
    half_mg = 0.5 * mg
    mc = own_row(mc_all_ref, n % groups, k, q, part)
    start = own_row(start_ref, n, k, q, part)
    def first(pair, _):
        for p in range(2):
            v = 2 * pair + p
            head = jnp.where(jnp.logical_and(v == 0, jnp.logical_and(sub == 0, part == 0)), start, 0.0)
            for m in range(SUB):
                got = got_ref[v * SUB + m].astype(jnp.float32)
                for g in range(2 * rows // SUB):
                    at = ((p * 2 * rows) + g * SUB + m) * SUB
                    flat[at : at + SUB, :] = got[g * SUB : (g + 1) * SUB]
            for r in range(rows):
                at = (p * 2 * rows + r // SUB * SUB) * SUB + r % SUB
                g = 0.5 * flat[pl.ds(at, SUB, stride=SUB), :]
                c = flat[pl.ds(at + rows * SUB, SUB, stride=SUB), :]
                if r == 0:
                    sl, of = coefficients(g, c, head, half_mg, mg, mc)
                    of -= sl * head
                    a, b = sl, of
                else:
                    sl, of = coefficients_at_zero(g, c, mg, mc)
                    a, b = sl * a, sl * b + of
                gate_ref[v, r] = g
                cand_ref[v, r] = c
                slopes_ref[v, r] = sl
                offset_ref[v, r] = of
            scale_ref[v] = a
            shift_ref[v] = b
        return 0

    def following(last, v, _):
        e = entry_ref[v]
        for r in range(rows):
            sl, at_slope = coefficients(gate_ref[v, r], cand_ref[v, r], e, half_mg, mg, mc)
            if last:
                a, b = (sl, at_slope - sl * e) if r == 0 else (sl * a, sl * (b - e) + at_slope)
            else:
                of = at_slope - sl * e
                a, b = (sl, of) if r == 0 else (sl * a, sl * b + of)
            if r < rows - 1:
                e = slopes_ref[v, r] * e + offset_ref[v, r]
            if not last:
                slopes_ref[v, r] = sl
                offset_ref[v, r] = of
        scale_ref[v] = a
        shift_ref[v] = b
        return 0

    def scan(v, state):
        a, b = scale_ref[v], shift_ref[v]
        for step in (1, 2):
            earlier_a = jnp.where(part >= step, roll_parts(a, step), 1.0)
            earlier_b = jnp.where(part >= step, roll_parts(b, step), 0.0)
            a, b = a * earlier_a, a * earlier_b + b
        part_a = jnp.where(part >= 1, roll_parts(a, 1), 1.0)
        part_b = jnp.where(part >= 1, roll_parts(b, 1), 0.0)
        a, b = repeat_last_part(a, part), repeat_last_part(b, part)
        for step in (1, 2, 4):
            earlier_a = jnp.where(sub >= step, pltpu.roll(a, step, 0), 1.0)
            earlier_b = jnp.where(sub >= step, pltpu.roll(b, step, 0), 0.0)
            a, b = a * earlier_a, a * earlier_b + b
        sub_a = jnp.where(sub >= 1, pltpu.roll(a, 1, 0), 1.0)
        sub_b = jnp.where(sub >= 1, pltpu.roll(b, 1, 0), 0.0)
        entry_ref[v] = part_a * (sub_a * state + sub_b) + part_b
        whole_a = jnp.broadcast_to(a[SUB - 1 : SUB], (SUB, LANES))
        whole_b = jnp.broadcast_to(b[SUB - 1 : SUB], (SUB, LANES))
        return whole_a * state + whole_b

    def entries(i):
        lax.fori_loop(0, tiles, scan, start, unroll=8)
        for v in range(tiles):
            at = v * SUB
            moved = roll_parts(entry_ref[v], i)
            out_ref[at : at + SUB, :] = moved if i == 0 else jnp.where(part == i, moved, out_ref[at : at + SUB, :])

    lax.fori_loop(0, tiles // 2, first, 0)
    entries(0)
    lax.fori_loop(0, tiles, functools.partial(following, False), 0, unroll=2)
    entries(1)
    lax.fori_loop(0, tiles, functools.partial(following, True), 0, unroll=2)
    entries(2)


def last_kernel(seqs, steps, groups, gate_ref, cand_ref, entry_ref, mg_ref, mc_ref, out_ref,
                gate_tmp, cand_tmp, out_tmp):
    part = lane_part()
    at_start = jnp.logical_and(lax.axis_index("tm") == 0, lax.axis_index("grp") == 0)
    head_scale = jnp.where(at_start, 1.0, 0.0)

    def entry_rows(n):
        got = [entry_ref[(n * PARTS + q) * SUB : (n * PARTS + q + 1) * SUB, :] for q in range(PARTS)]
        rows = []
        for i in range(3):
            row = roll_parts(got[0], -i)
            for q in range(1, PARTS):
                row = jnp.where(part == q, roll_parts(got[q], q - i), row)
            rows.append(row)
        return tuple(rows)

    def block(s, i, states, begin):
        at = i * SUB if isinstance(i, int) else pl.multiple_of(i * SUB, SUB)
        done = []
        for j in range(groups):
            for k in range(SUB):
                lane = j * GROUP + k * LANES
                row = (j * SUB + k) * SUB
                gate = gate_ref[s, pl.ds(at, SUB), lane : lane + LANES].astype(jnp.float32)
                gate_tmp[row : row + SUB, :] = 0.5 * gate
                cand_tmp[row : row + SUB, :] = cand_ref[s, pl.ds(at, SUB), lane : lane + LANES].astype(jnp.float32)
        for j in range(groups):
            mg, mc = mg_ref[j], mc_ref[j]
            half_mg = 0.5 * mg
            first, second, third = states[j]
            for t in range(SUB):
                window = pl.ds(j * SUB * SUB + t, SUB, stride=SUB)
                g, c = gate_tmp[window, :], cand_tmp[window, :]
                sl2, at2 = coefficients(g, c, first, half_mg, mg, mc)
                sl3, at3 = coefficients(g, c, second, half_mg, mg, mc)
                third = sl3 * (third - second) + at3
                second = sl2 * (second - first) + at2
                if begin and t == 0:
                    head = first * head_scale
                    sl1, at1 = coefficients(g, c, head, half_mg, mg, mc)
                    first = sl1 * (first - head) + at1
                else:
                    sl1, at1 = coefficients_at_zero(g, c, mg, mc)
                    first = sl1 * first + at1
                row = (j * SUB + t) * SUB
                out_tmp[row : row + SUB, :] = third
            done.append((first, second, third))
            for k in range(SUB):
                lane = j * GROUP + k * LANES
                rows = out_tmp[pl.ds(j * SUB * SUB + k, SUB, stride=SUB), :]
                out_ref[s, pl.ds(at, SUB), lane : lane + LANES] = rows.astype(jnp.bfloat16)
        return tuple(done)

    for s in range(seqs):
        states = tuple(entry_rows(s * groups + j) for j in range(groups))
        states = block(s, 0, states, True)
        lax.fori_loop(1, steps // SUB, lambda i, c: block(s, i, c, False), states)


def call(kernel, outs, scratch, *args, vmem=32, space=pltpu.VMEM):
    spec = pl.BlockSpec(memory_space=space)
    return pl.pallas_call(
        kernel,
        out_shape=outs,
        in_specs=[spec] * len(args),
        out_specs=jax.tree.map(lambda _: spec, outs),
        scratch_shapes=scratch,
        compiler_params=pltpu.CompilerParams(vmem_limit_bytes=vmem * 2**20),
    )(*args)


def on_device(gate_pre, cand_pre, start_state, mix_gate, mix_cand):
    seqs, steps, width = gate_pre.shape
    groups = width // GROUP
    slabs = seqs * groups
    axes = ("tm", "grp")
    owners = lax.axis_size(axes)
    rows = steps // PARTS
    tiles = owners // SUB
    f32 = functools.partial(jax.ShapeDtypeStruct, dtype=jnp.float32)

    def scratch(*shape):
        return pltpu.VMEM(shape, jnp.float32)

    mg = mix_gate.reshape(groups, SUB, LANES)
    mc = mix_cand.reshape(groups, SUB, LANES)
    packed = call(
        functools.partial(pack_kernel, seqs, steps, groups),
        jax.ShapeDtypeStruct((owners, 2 * rows, LANES), jnp.bfloat16),
        [pltpu.VMEM((slabs, steps, GROUP), jnp.bfloat16), pltpu.VMEM((slabs, steps, GROUP), jnp.bfloat16),
         pltpu.VMEM((owners, 2 * rows, LANES), jnp.bfloat16),
         scratch(SUB * steps, LANES), scratch(SUB * steps, LANES), scratch(PARTS * 2 * rows * SUB, LANES),
         pltpu.SemaphoreType.DMA((2, slabs)), pltpu.SemaphoreType.DMA((slabs,))],
        gate_pre, cand_pre, vmem=56, space=pltpu.HBM)
    start = start_state.reshape(slabs, SUB, LANES)
    got = lax.all_to_all(packed, axes, 0, 0, tiled=True)
    tmp = scratch(groups * SUB * SUB, LANES)
    states = call(
        functools.partial(owner_kernel, groups, tiles, rows), f32((owners, LANES)),
        [scratch(2 * 2 * rows * SUB, LANES), *[scratch(tiles, rows, SUB, LANES)] * 4,
         scratch(tiles, SUB, LANES), scratch(tiles, SUB, LANES), scratch(tiles, SUB, LANES)],
        got, start, mg, mc, vmem=16)
    entry = lax.all_to_all(states.reshape(owners, 1, LANES), axes, 0, 0, tiled=True).reshape(owners, LANES)
    return call(
        functools.partial(last_kernel, seqs, steps, groups),
        jax.ShapeDtypeStruct(gate_pre.shape, jnp.bfloat16), [tmp, tmp, tmp],
        gate_pre, cand_pre, entry, mg, mc, vmem=16)


def solution(mesh):
    time = P(None, ("tm", "grp"), None)
    return jax.shard_map(
        on_device, mesh=mesh, in_specs=(time, time, P(), P(), P()), out_specs=time, check_vma=False
    )
```

```python
import functools

import jax
import jax.numpy as jnp
from jax import lax
from jax.experimental import pallas as pl
from jax.experimental.pallas import tpu as pltpu
from jax.sharding import PartitionSpec as P

LANES = 128
SUB = 8
PARTS = 4
WIDE = LANES // PARTS
GROUP = SUB * LANES


def forget_and_rest(half_gate):
    half = 0.5 * jnp.tanh(half_gate)
    return 0.5 + half, 0.5 - half


def coefficients(half_gate, cand_in, previous, half_mix_gate, mix_gate, mix_cand):
    forget, rest = forget_and_rest(half_gate + half_mix_gate * previous)
    candidate = jnp.tanh(cand_in + mix_cand * previous)
    kept = forget * (previous - candidate)
    slopes = forget + rest * (kept * mix_gate + (mix_cand - candidate * candidate * mix_cand))
    return slopes, candidate + kept


def coefficients_at_zero(half_gate, cand_in, mix_gate, mix_cand):
    forget, rest = forget_and_rest(half_gate)
    candidate = jnp.tanh(cand_in)
    kept = forget * candidate
    slopes = forget + rest * ((mix_cand - candidate * candidate * mix_cand) - kept * mix_gate)
    return slopes, candidate - kept


def lane_part():
    return lax.broadcasted_iota(jnp.int32, (SUB, LANES), 1) // WIDE


def roll_parts(x, parts):
    parts %= PARTS
    return pltpu.roll(x, parts * WIDE, 1) if parts else x


def pack_kernel(seqs, steps, groups, gate_hbm, cand_hbm, out_hbm,
                gate_ref, cand_ref, packed, gate_flat, cand_flat, mixed, x_ref, perm_ref, in_sem, out_sem):
    rows = steps // PARTS
    owners = PARTS * SUB
    slabs = seqs * groups

    def fetch(n):
        s, lane = n // groups, pl.multiple_of((n % groups) * GROUP, GROUP)
        window = (s, slice(None), pl.ds(lane, GROUP))
        return [
            pltpu.make_async_copy(gate_hbm.at[window], gate_ref.at[n], in_sem.at[0, n]),
            pltpu.make_async_copy(cand_hbm.at[window], cand_ref.at[n], in_sem.at[1, n]),
        ]

    def store(n):
        at = pl.multiple_of(n * owners, owners)
        return pltpu.make_async_copy(packed.at[pl.ds(at, owners)], out_hbm.at[pl.ds(at, owners)], out_sem.at[n])

    for n in range(slabs):
        for copy in fetch(n):
            copy.start()

    i = lax.broadcasted_iota(jnp.int32, perm_ref.shape, 0)
    target = i % LANES // WIDE * LANES + i // LANES * WIDE + i % WIDE
    perm_ref[...] = jnp.where(lax.broadcasted_iota(jnp.int32, perm_ref.shape, 1) == target, 1.0, 0.0).astype(jnp.bfloat16)

    def slab(n, _):
        for copy in fetch(n):
            copy.wait()
        for half, (in_ref, flat) in enumerate(((gate_ref, gate_flat), (cand_ref, cand_flat))):
            for i in range(steps // SUB):
                for k in range(SUB):
                    at = (i * SUB + k) * SUB
                    flat[at : at + SUB, :] = in_ref[
                        n, i * SUB : (i + 1) * SUB, k * LANES : (k + 1) * LANES].astype(jnp.float32)
            for r in range(0, rows, 2):
                for u in range(PARTS):
                    two = []
                    for t in (u * rows + r, u * rows + r + 1):
                        two.append(flat[pl.ds(t // SUB * SUB * SUB + t % SUB, SUB, stride=SUB), :])
                    at = (half * rows + r) * SUB
                    x_ref[at : at + 2 * SUB, u * LANES : (u + 1) * LANES] = jnp.concatenate(
                        two, axis=0).astype(jnp.bfloat16)
        moved = jnp.dot(x_ref[...], perm_ref[...], preferred_element_type=jnp.float32)
        for q in range(PARTS):
            at = q * 2 * rows * SUB
            mixed[at : at + 2 * rows * SUB, :] = moved[:, q * LANES : (q + 1) * LANES]
        for q in range(PARTS):
            for k in range(SUB):
                for g in range(rows // SUB):
                    at = (q * 2 * rows + g * 2 * SUB) * SUB + k
                    two = [mixed[pl.ds(at + h * SUB * SUB, SUB, stride=SUB), :] for h in range(2)]
                    packed[n * owners + q * SUB + k, g * 2 * SUB : (g + 1) * 2 * SUB, :] = jnp.concatenate(
                        two, axis=0).astype(jnp.bfloat16)
        store(n).start()
        return 0

    lax.fori_loop(0, slabs, slab, 0)
    for n in range(slabs):
        store(n).wait()


def repeat_first_part(x, part):
    x = jnp.where(part == 0, x, roll_parts(x, 1))
    return jnp.where(part < 2, x, roll_parts(x, 2))


def own_row(ref, n, k, q, part):
    row = jnp.broadcast_to(ref[n, pl.ds(k, 1), :], (SUB, LANES))
    return repeat_first_part(pltpu.roll(row, ((PARTS - q) % PARTS) * WIDE, 1), part)


def owner_kernel(groups, tiles, rows, got_ref, start_ref, mg_all_ref, mc_all_ref, out_ref,
                 flat, gate_ref, cand_ref, slopes_ref, offset_ref, scale_ref, shift_ref, entry_ref):
    part = lane_part()
    sub = lax.broadcasted_iota(jnp.int32, (SUB, LANES), 0)
    owner = lax.axis_index("tm") * lax.axis_size("grp") + lax.axis_index("grp")
    n, q, k = owner // (PARTS * SUB), (owner // SUB) % PARTS, owner % SUB
    mg = own_row(mg_all_ref, n % groups, k, q, part)
    half_mg = 0.5 * mg
    mc = own_row(mc_all_ref, n % groups, k, q, part)
    start = own_row(start_ref, n, k, q, part)
    def first(pair, _):
        for p in range(2):
            v = 2 * pair + p
            head = jnp.where(jnp.logical_and(v == 0, jnp.logical_and(sub == 0, part == 0)), start, 0.0)
            for m in range(SUB):
                got = got_ref[v * SUB + m].astype(jnp.float32)
                for g in range(2 * rows // SUB):
                    at = ((p * 2 * rows) + g * SUB + m) * SUB
                    flat[at : at + SUB, :] = got[g * SUB : (g + 1) * SUB]
            for r in range(rows):
                at = (p * 2 * rows + r // SUB * SUB) * SUB + r % SUB
                g = 0.5 * flat[pl.ds(at, SUB, stride=SUB), :]
                c = flat[pl.ds(at + rows * SUB, SUB, stride=SUB), :]
                if r == 0:
                    sl, of = coefficients(g, c, head, half_mg, mg, mc)
                    of -= sl * head
                    a, b = sl, of
                else:
                    sl, of = coefficients_at_zero(g, c, mg, mc)
                    a, b = sl * a, sl * b + of
                gate_ref[v, r] = g
                cand_ref[v, r] = c
                slopes_ref[v, r] = sl
                offset_ref[v, r] = of
            scale_ref[v] = a
            shift_ref[v] = b
        return 0

    def following(last, v, _):
        e = entry_ref[v]
        for r in range(rows):
            sl, at_slope = coefficients(gate_ref[v, r], cand_ref[v, r], e, half_mg, mg, mc)
            if last:
                a, b = (sl, at_slope - sl * e) if r == 0 else (sl * a, sl * (b - e) + at_slope)
            else:
                of = at_slope - sl * e
                a, b = (sl, of) if r == 0 else (sl * a, sl * b + of)
            if r < rows - 1:
                e = slopes_ref[v, r] * e + offset_ref[v, r]
            if not last:
                slopes_ref[v, r] = sl
                offset_ref[v, r] = of
        scale_ref[v] = a
        shift_ref[v] = b
        return 0

    def scan(v, state):
        a, b = scale_ref[v], shift_ref[v]
        turned = [(roll_parts(a, step), roll_parts(b, step)) for step in range(PARTS)]
        part_a, part_b = 1.0, 0.0
        for step in (3, 2, 1):
            earlier_a = jnp.where(part >= step, turned[step][0], 1.0)
            earlier_b = jnp.where(part >= step, turned[step][1], 0.0)
            part_a, part_b = earlier_a * part_a, earlier_a * part_b + earlier_b
        a, b = a * part_a, a * part_b + b
        for step in (3, 2, 1):
            later_a = jnp.where(part < step, turned[step][0], 1.0)
            later_b = jnp.where(part < step, turned[step][1], 0.0)
            a, b = later_a * a, later_a * b + later_b
        for step in (1, 2, 4):
            earlier_a = jnp.where(sub >= step, pltpu.roll(a, step, 0), 1.0)
            earlier_b = jnp.where(sub >= step, pltpu.roll(b, step, 0), 0.0)
            a, b = a * earlier_a, a * earlier_b + b
        sub_a = jnp.where(sub >= 1, pltpu.roll(a, 1, 0), 1.0)
        sub_b = jnp.where(sub >= 1, pltpu.roll(b, 1, 0), 0.0)
        entry_ref[v] = part_a * (sub_a * state + sub_b) + part_b
        whole_a = jnp.broadcast_to(a[SUB - 1 : SUB], (SUB, LANES))
        whole_b = jnp.broadcast_to(b[SUB - 1 : SUB], (SUB, LANES))
        return whole_a * state + whole_b

    def entries(i):
        lax.fori_loop(0, tiles, scan, start, unroll=8)
        for v in range(tiles):
            at = v * SUB
            moved = roll_parts(entry_ref[v], i)
            out_ref[at : at + SUB, :] = moved if i == 0 else jnp.where(part == i, moved, out_ref[at : at + SUB, :])

    lax.fori_loop(0, tiles // 2, first, 0)
    entries(0)
    lax.fori_loop(0, tiles, functools.partial(following, False), 0, unroll=2)
    entries(1)
    lax.fori_loop(0, tiles, functools.partial(following, True), 0, unroll=2)
    entries(2)


def last_kernel(seqs, steps, groups, gate_ref, cand_ref, entry_ref, mg_ref, mc_ref, out_ref,
                gate_tmp, cand_tmp, out_tmp):
    part = lane_part()
    at_start = jnp.logical_and(lax.axis_index("tm") == 0, lax.axis_index("grp") == 0)
    head_scale = jnp.where(at_start, 1.0, 0.0)

    def entry_rows(n):
        got = [entry_ref[(n * PARTS + q) * SUB : (n * PARTS + q + 1) * SUB, :] for q in range(PARTS)]
        rows = []
        for i in range(3):
            row = roll_parts(got[0], -i)
            for q in range(1, PARTS):
                row = jnp.where(part == q, roll_parts(got[q], q - i), row)
            rows.append(row)
        return tuple(rows)

    def block(s, i, states, begin):
        at = i * SUB if isinstance(i, int) else pl.multiple_of(i * SUB, SUB)
        done = []
        for j in range(groups):
            for k in range(SUB):
                lane = j * GROUP + k * LANES
                row = (j * SUB + k) * SUB
                gate = gate_ref[s, pl.ds(at, SUB), lane : lane + LANES].astype(jnp.float32)
                gate_tmp[row : row + SUB, :] = 0.5 * gate
                cand_tmp[row : row + SUB, :] = cand_ref[s, pl.ds(at, SUB), lane : lane + LANES].astype(jnp.float32)
        for j in range(groups):
            mg, mc = mg_ref[j], mc_ref[j]
            half_mg = 0.5 * mg
            first, second, third = states[j]
            for t in range(SUB):
                window = pl.ds(j * SUB * SUB + t, SUB, stride=SUB)
                g, c = gate_tmp[window, :], cand_tmp[window, :]
                sl2, at2 = coefficients(g, c, first, half_mg, mg, mc)
                sl3, at3 = coefficients(g, c, second, half_mg, mg, mc)
                third = sl3 * (third - second) + at3
                second = sl2 * (second - first) + at2
                if begin and t == 0:
                    head = first * head_scale
                    sl1, at1 = coefficients(g, c, head, half_mg, mg, mc)
                    first = sl1 * (first - head) + at1
                else:
                    sl1, at1 = coefficients_at_zero(g, c, mg, mc)
                    first = sl1 * first + at1
                row = (j * SUB + t) * SUB
                out_tmp[row : row + SUB, :] = third
            done.append((first, second, third))
            for k in range(SUB):
                lane = j * GROUP + k * LANES
                rows = out_tmp[pl.ds(j * SUB * SUB + k, SUB, stride=SUB), :]
                out_ref[s, pl.ds(at, SUB), lane : lane + LANES] = rows.astype(jnp.bfloat16)
        return tuple(done)

    for s in range(seqs):
        states = tuple(entry_rows(s * groups + j) for j in range(groups))
        states = block(s, 0, states, True)
        lax.fori_loop(1, steps // SUB, lambda i, c: block(s, i, c, False), states)


def call(kernel, outs, scratch, *args, vmem=32, space=pltpu.VMEM):
    spec = pl.BlockSpec(memory_space=space)
    return pl.pallas_call(
        kernel,
        out_shape=outs,
        in_specs=[spec] * len(args),
        out_specs=jax.tree.map(lambda _: spec, outs),
        scratch_shapes=scratch,
        compiler_params=pltpu.CompilerParams(vmem_limit_bytes=vmem * 2**20),
    )(*args)


def on_device(gate_pre, cand_pre, start_state, mix_gate, mix_cand):
    seqs, steps, width = gate_pre.shape
    groups = width // GROUP
    slabs = seqs * groups
    axes = ("tm", "grp")
    owners = lax.axis_size(axes)
    rows = steps // PARTS
    tiles = owners // SUB
    f32 = functools.partial(jax.ShapeDtypeStruct, dtype=jnp.float32)

    def scratch(*shape):
        return pltpu.VMEM(shape, jnp.float32)

    mg = mix_gate.reshape(groups, SUB, LANES)
    mc = mix_cand.reshape(groups, SUB, LANES)
    packed = call(
        functools.partial(pack_kernel, seqs, steps, groups),
        jax.ShapeDtypeStruct((owners, 2 * rows, LANES), jnp.bfloat16),
        [pltpu.VMEM((slabs, steps, GROUP), jnp.bfloat16), pltpu.VMEM((slabs, steps, GROUP), jnp.bfloat16),
         pltpu.VMEM((owners, 2 * rows, LANES), jnp.bfloat16),
         scratch(SUB * steps, LANES), scratch(SUB * steps, LANES), scratch(PARTS * 2 * rows * SUB, LANES),
         pltpu.VMEM((2 * rows * SUB, PARTS * LANES), jnp.bfloat16),
         pltpu.VMEM((PARTS * LANES, PARTS * LANES), jnp.bfloat16),
         pltpu.SemaphoreType.DMA((2, slabs)), pltpu.SemaphoreType.DMA((slabs,))],
        gate_pre, cand_pre, vmem=56, space=pltpu.HBM)
    start = start_state.reshape(slabs, SUB, LANES)
    got = lax.all_to_all(packed, axes, 0, 0, tiled=True)
    tmp = scratch(groups * SUB * SUB, LANES)
    states = call(
        functools.partial(owner_kernel, groups, tiles, rows), f32((owners, LANES)),
        [scratch(2 * 2 * rows * SUB, LANES), *[scratch(tiles, rows, SUB, LANES)] * 4,
         scratch(tiles, SUB, LANES), scratch(tiles, SUB, LANES), scratch(tiles, SUB, LANES)],
        got, start, mg, mc, vmem=16)
    entry = lax.all_to_all(states.reshape(owners, 1, LANES), axes, 0, 0, tiled=True).reshape(owners, LANES)
    return call(
        functools.partial(last_kernel, seqs, steps, groups),
        jax.ShapeDtypeStruct(gate_pre.shape, jnp.bfloat16), [tmp, tmp, tmp],
        gate_pre, cand_pre, entry, mg, mc, vmem=16)


def solution(mesh):
    time = P(None, ("tm", "grp"), None)
    return jax.shard_map(
        on_device, mesh=mesh, in_specs=(time, time, P(), P(), P()), out_specs=time, check_vma=False
    )
```

```python
import functools

import jax
import jax.numpy as jnp
from jax import lax
from jax.experimental import pallas as pl
from jax.experimental.pallas import tpu as pltpu
from jax.sharding import PartitionSpec as P

LANES = 128
SUB = 8
PARTS = 4
WIDE = LANES // PARTS
GROUP = SUB * LANES


def forget_and_rest(half_gate):
    half = 0.5 * jnp.tanh(half_gate)
    return 0.5 + half, 0.5 - half


def coefficients(half_gate, cand_in, previous, half_mix_gate, mix_gate, mix_cand):
    forget, rest = forget_and_rest(half_gate + half_mix_gate * previous)
    candidate = jnp.tanh(cand_in + mix_cand * previous)
    kept = forget * (previous - candidate)
    slopes = forget + rest * (kept * mix_gate + (mix_cand - candidate * candidate * mix_cand))
    return slopes, candidate + kept


def coefficients_at_zero(half_gate, cand_in, mix_gate, mix_cand):
    forget, rest = forget_and_rest(half_gate)
    candidate = jnp.tanh(cand_in)
    kept = forget * candidate
    slopes = forget + rest * ((mix_cand - candidate * candidate * mix_cand) - kept * mix_gate)
    return slopes, candidate - kept


def lane_part():
    return lax.broadcasted_iota(jnp.int32, (SUB, LANES), 1) // WIDE


def roll_parts(x, parts):
    parts %= PARTS
    return pltpu.roll(x, parts * WIDE, 1) if parts else x


def pack_kernel(seqs, steps, groups, gate_hbm, cand_hbm, out_hbm,
                gate_ref, cand_ref, packed, gate_flat, cand_flat, mixed, x_ref, perm_ref, in_sem, out_sem):
    rows = steps // PARTS
    owners = PARTS * SUB
    slabs = seqs * groups

    def fetch(n):
        s, lane = n // groups, pl.multiple_of((n % groups) * GROUP, GROUP)
        window = (s, slice(None), pl.ds(lane, GROUP))
        return [
            pltpu.make_async_copy(gate_hbm.at[window], gate_ref.at[n], in_sem.at[0, n]),
            pltpu.make_async_copy(cand_hbm.at[window], cand_ref.at[n], in_sem.at[1, n]),
        ]

    def store(n):
        at = pl.multiple_of(n * owners, owners)
        return pltpu.make_async_copy(packed.at[pl.ds(at, owners)], out_hbm.at[pl.ds(at, owners)], out_sem.at[n])

    for n in range(slabs):
        for copy in fetch(n):
            copy.start()

    i = lax.broadcasted_iota(jnp.int32, perm_ref.shape, 0)
    target = i % LANES // WIDE * LANES + i // LANES * WIDE + i % WIDE
    perm_ref[...] = jnp.where(lax.broadcasted_iota(jnp.int32, perm_ref.shape, 1) == target, 1.0, 0.0).astype(jnp.bfloat16)

    def slab(n, _):
        for copy in fetch(n):
            copy.wait()
        for half, (in_ref, flat) in enumerate(((gate_ref, gate_flat), (cand_ref, cand_flat))):
            for i in range(steps // SUB):
                for k in range(SUB):
                    at = (i * SUB + k) * SUB
                    flat[at : at + SUB, :] = in_ref[
                        n, i * SUB : (i + 1) * SUB, k * LANES : (k + 1) * LANES].astype(jnp.float32)
            for r in range(0, rows, 2):
                for u in range(PARTS):
                    two = []
                    for t in (u * rows + r, u * rows + r + 1):
                        two.append(flat[pl.ds(t // SUB * SUB * SUB + t % SUB, SUB, stride=SUB), :])
                    at = (half * rows + r) * SUB
                    x_ref[at : at + 2 * SUB, u * LANES : (u + 1) * LANES] = jnp.concatenate(
                        two, axis=0).astype(jnp.bfloat16)
        moved = jnp.dot(x_ref[...], perm_ref[...], preferred_element_type=jnp.float32)
        for q in range(PARTS):
            at = q * 2 * rows * SUB
            mixed[at : at + 2 * rows * SUB, :] = moved[:, q * LANES : (q + 1) * LANES]
        for q in range(PARTS):
            for k in range(SUB):
                for g in range(rows // SUB):
                    at = (q * 2 * rows + g * 2 * SUB) * SUB + k
                    two = [mixed[pl.ds(at + h * SUB * SUB, SUB, stride=SUB), :] for h in range(2)]
                    packed[n * owners + q * SUB + k, g * 2 * SUB : (g + 1) * 2 * SUB, :] = jnp.concatenate(
                        two, axis=0).astype(jnp.bfloat16)
        store(n).start()
        return 0

    lax.fori_loop(0, slabs, slab, 0)
    for n in range(slabs):
        store(n).wait()


def repeat_first_part(x, part):
    x = jnp.where(part == 0, x, roll_parts(x, 1))
    return jnp.where(part < 2, x, roll_parts(x, 2))


def own_row(ref, n, k, q, part):
    row = jnp.broadcast_to(ref[n, pl.ds(k, 1), :], (SUB, LANES))
    return repeat_first_part(pltpu.roll(row, ((PARTS - q) % PARTS) * WIDE, 1), part)


def owner_kernel(groups, tiles, rows, got_ref, start_ref, mg_all_ref, mc_all_ref, out_ref,
                 flat, gate_ref, cand_ref, slopes_ref, offset_ref, scale_ref, shift_ref, entry_ref):
    part = lane_part()
    sub = lax.broadcasted_iota(jnp.int32, (SUB, LANES), 0)
    owner = lax.axis_index("tm") * lax.axis_size("grp") + lax.axis_index("grp")
    n, q, k = owner // (PARTS * SUB), (owner // SUB) % PARTS, owner % SUB
    mg = own_row(mg_all_ref, n % groups, k, q, part)
    half_mg = 0.5 * mg
    mc = own_row(mc_all_ref, n % groups, k, q, part)
    start = own_row(start_ref, n, k, q, part)
    def first(pair, _):
        for p in range(2):
            v = 2 * pair + p
            head = jnp.where(jnp.logical_and(v == 0, jnp.logical_and(sub == 0, part == 0)), start, 0.0)
            for m in range(SUB):
                got = got_ref[v * SUB + m].astype(jnp.float32)
                for g in range(2 * rows // SUB):
                    at = ((p * 2 * rows) + g * SUB + m) * SUB
                    flat[at : at + SUB, :] = got[g * SUB : (g + 1) * SUB]
            for r in range(rows):
                at = (p * 2 * rows + r // SUB * SUB) * SUB + r % SUB
                g = 0.5 * flat[pl.ds(at, SUB, stride=SUB), :]
                c = flat[pl.ds(at + rows * SUB, SUB, stride=SUB), :]
                if r == 0:
                    sl, of = coefficients(g, c, head, half_mg, mg, mc)
                    of -= sl * head
                    a, b = sl, of
                else:
                    sl, of = coefficients_at_zero(g, c, mg, mc)
                    a, b = sl * a, sl * b + of
                gate_ref[v, r] = g
                cand_ref[v, r] = c
                slopes_ref[v, r] = sl
                offset_ref[v, r] = of
            scale_ref[v] = a
            shift_ref[v] = b
        return 0

    def following(last, v, _):
        e = entry_ref[v]
        for r in range(rows):
            sl, at_slope = coefficients(gate_ref[v, r], cand_ref[v, r], e, half_mg, mg, mc)
            if last:
                a, b = (sl, at_slope - sl * e) if r == 0 else (sl * a, sl * (b - e) + at_slope)
            else:
                of = at_slope - sl * e
                a, b = (sl, of) if r == 0 else (sl * a, sl * b + of)
            if r < rows - 1:
                e = slopes_ref[v, r] * e + offset_ref[v, r]
            if not last:
                slopes_ref[v, r] = sl
                offset_ref[v, r] = of
        scale_ref[v] = a
        shift_ref[v] = b
        return 0

    def scan(v, state):
        a, b = scale_ref[v], shift_ref[v]
        turned = [(roll_parts(a, step), roll_parts(b, step)) for step in range(PARTS)]
        part_a, part_b = 1.0, 0.0
        for step in (3, 2, 1):
            earlier_a = jnp.where(part >= step, turned[step][0], 1.0)
            earlier_b = jnp.where(part >= step, turned[step][1], 0.0)
            part_a, part_b = earlier_a * part_a, earlier_a * part_b + earlier_b
        a, b = a * part_a, a * part_b + b
        for step in (3, 2, 1):
            later_a = jnp.where(part < step, turned[step][0], 1.0)
            later_b = jnp.where(part < step, turned[step][1], 0.0)
            a, b = later_a * a, later_a * b + later_b
        for step in (1, 2, 4):
            earlier_a = jnp.where(sub >= step, pltpu.roll(a, step, 0), 1.0)
            earlier_b = jnp.where(sub >= step, pltpu.roll(b, step, 0), 0.0)
            a, b = a * earlier_a, a * earlier_b + b
        sub_a = jnp.where(sub >= 1, pltpu.roll(a, 1, 0), 1.0)
        sub_b = jnp.where(sub >= 1, pltpu.roll(b, 1, 0), 0.0)
        entry_ref[v] = part_a * (sub_a * state + sub_b) + part_b
        whole_a = jnp.broadcast_to(a[SUB - 1 : SUB], (SUB, LANES))
        whole_b = jnp.broadcast_to(b[SUB - 1 : SUB], (SUB, LANES))
        return whole_a * state + whole_b

    def entries(i):
        lax.fori_loop(0, tiles, scan, start, unroll=32)
        for v in range(tiles):
            at = v * SUB
            moved = roll_parts(entry_ref[v], i)
            out_ref[at : at + SUB, :] = moved if i == 0 else jnp.where(part == i, moved, out_ref[at : at + SUB, :])

    lax.fori_loop(0, tiles // 2, first, 0)
    entries(0)
    lax.fori_loop(0, tiles, functools.partial(following, False), 0, unroll=4)
    entries(1)
    lax.fori_loop(0, tiles, functools.partial(following, True), 0, unroll=4)
    entries(2)


def last_kernel(seqs, steps, groups, gate_ref, cand_ref, entry_ref, mg_ref, mc_ref, out_hbm,
                out_ref, gate_tmp, cand_tmp, out_tmp, out_sem):
    part = lane_part()

    def store(s, i):
        window = (s, pl.ds(i * SUB if isinstance(i, int) else pl.multiple_of(i * SUB, SUB), SUB))
        return pltpu.make_async_copy(out_ref.at[window], out_hbm.at[window], out_sem.at[s, i])

    at_start = jnp.logical_and(lax.axis_index("tm") == 0, lax.axis_index("grp") == 0)
    head_scale = jnp.where(at_start, 1.0, 0.0)

    def entry_rows(n):
        got = [entry_ref[(n * PARTS + q) * SUB : (n * PARTS + q + 1) * SUB, :] for q in range(PARTS)]
        rows = []
        for i in range(3):
            row = roll_parts(got[0], -i)
            for q in range(1, PARTS):
                row = jnp.where(part == q, roll_parts(got[q], q - i), row)
            rows.append(row)
        return tuple(rows)

    def block(s, i, states, begin):
        at = i * SUB if isinstance(i, int) else pl.multiple_of(i * SUB, SUB)
        done = []
        for j in range(groups):
            for k in range(SUB):
                lane = j * GROUP + k * LANES
                row = (j * SUB + k) * SUB
                gate = gate_ref[s, pl.ds(at, SUB), lane : lane + LANES].astype(jnp.float32)
                gate_tmp[row : row + SUB, :] = 0.5 * gate
                cand_tmp[row : row + SUB, :] = cand_ref[s, pl.ds(at, SUB), lane : lane + LANES].astype(jnp.float32)
        for j in range(groups):
            mg, mc = mg_ref[j], mc_ref[j]
            half_mg = 0.5 * mg
            first, second, third = states[j]
            for t in range(SUB):
                window = pl.ds(j * SUB * SUB + t, SUB, stride=SUB)
                g, c = gate_tmp[window, :], cand_tmp[window, :]
                sl2, at2 = coefficients(g, c, first, half_mg, mg, mc)
                sl3, at3 = coefficients(g, c, second, half_mg, mg, mc)
                third = sl3 * (third - second) + at3
                second = sl2 * (second - first) + at2
                if begin and t == 0:
                    head = first * head_scale
                    sl1, at1 = coefficients(g, c, head, half_mg, mg, mc)
                    first = sl1 * (first - head) + at1
                else:
                    sl1, at1 = coefficients_at_zero(g, c, mg, mc)
                    first = sl1 * first + at1
                row = (j * SUB + t) * SUB
                out_tmp[row : row + SUB, :] = third
            done.append((first, second, third))
            for k in range(SUB):
                lane = j * GROUP + k * LANES
                rows = out_tmp[pl.ds(j * SUB * SUB + k, SUB, stride=SUB), :]
                out_ref[s, pl.ds(at, SUB), lane : lane + LANES] = rows.astype(jnp.bfloat16)
        store(s, i).start()
        return tuple(done)

    for s in range(seqs):
        states = tuple(entry_rows(s * groups + j) for j in range(groups))
        states = block(s, 0, states, True)
        lax.fori_loop(1, steps // SUB, lambda i, c: block(s, i, c, False), states)
    for s in range(seqs):
        for i in range(steps // SUB):
            store(s, i).wait()


def call(kernel, outs, scratch, *args, vmem=32, space=pltpu.VMEM, out_space=None):
    spec = pl.BlockSpec(memory_space=space)
    out_spec = pl.BlockSpec(memory_space=out_space or space)
    return pl.pallas_call(
        kernel,
        out_shape=outs,
        in_specs=[spec] * len(args),
        out_specs=jax.tree.map(lambda _: out_spec, outs),
        scratch_shapes=scratch,
        compiler_params=pltpu.CompilerParams(vmem_limit_bytes=vmem * 2**20),
    )(*args)


def on_device(gate_pre, cand_pre, start_state, mix_gate, mix_cand):
    seqs, steps, width = gate_pre.shape
    groups = width // GROUP
    slabs = seqs * groups
    axes = ("tm", "grp")
    owners = lax.axis_size(axes)
    rows = steps // PARTS
    tiles = owners // SUB
    f32 = functools.partial(jax.ShapeDtypeStruct, dtype=jnp.float32)

    def scratch(*shape):
        return pltpu.VMEM(shape, jnp.float32)

    mg = mix_gate.reshape(groups, SUB, LANES)
    mc = mix_cand.reshape(groups, SUB, LANES)
    packed = call(
        functools.partial(pack_kernel, seqs, steps, groups),
        jax.ShapeDtypeStruct((owners, 2 * rows, LANES), jnp.bfloat16),
        [pltpu.VMEM((slabs, steps, GROUP), jnp.bfloat16), pltpu.VMEM((slabs, steps, GROUP), jnp.bfloat16),
         pltpu.VMEM((owners, 2 * rows, LANES), jnp.bfloat16),
         scratch(SUB * steps, LANES), scratch(SUB * steps, LANES), scratch(PARTS * 2 * rows * SUB, LANES),
         pltpu.VMEM((2 * rows * SUB, PARTS * LANES), jnp.bfloat16),
         pltpu.VMEM((PARTS * LANES, PARTS * LANES), jnp.bfloat16),
         pltpu.SemaphoreType.DMA((2, slabs)), pltpu.SemaphoreType.DMA((slabs,))],
        gate_pre, cand_pre, vmem=56, space=pltpu.HBM)
    start = start_state.reshape(slabs, SUB, LANES)
    got = lax.all_to_all(packed, axes, 0, 0, tiled=True)
    tmp = scratch(groups * SUB * SUB, LANES)
    states = call(
        functools.partial(owner_kernel, groups, tiles, rows), f32((owners, LANES)),
        [scratch(2 * 2 * rows * SUB, LANES), *[scratch(tiles, rows, SUB, LANES)] * 4,
         scratch(tiles, SUB, LANES), scratch(tiles, SUB, LANES), scratch(tiles, SUB, LANES)],
        got, start, mg, mc, vmem=16)
    entry = lax.all_to_all(states.reshape(owners, 1, LANES), axes, 0, 0, tiled=True).reshape(owners, LANES)
    return call(
        functools.partial(last_kernel, seqs, steps, groups),
        jax.ShapeDtypeStruct(gate_pre.shape, jnp.bfloat16),
        [pltpu.VMEM(gate_pre.shape, jnp.bfloat16), tmp, tmp, tmp, pltpu.SemaphoreType.DMA((seqs, steps // SUB))],
        gate_pre, cand_pre, entry, mg, mc, vmem=16, out_space=pltpu.HBM)


def solution(mesh):
    time = P(None, ("tm", "grp"), None)
    return jax.shard_map(
        on_device, mesh=mesh, in_specs=(time, time, P(), P(), P()), out_specs=time, check_vma=False
    )
```

```python
import functools

import jax
import jax.numpy as jnp
from jax import lax
from jax.experimental import pallas as pl
from jax.experimental.pallas import tpu as pltpu
from jax.sharding import PartitionSpec as P

LANES = 128
SUB = 8
PARTS = 4
WIDE = LANES // PARTS
GROUP = SUB * LANES


def forget_and_rest(half_gate):
    half = 0.5 * jnp.tanh(half_gate)
    return 0.5 + half, 0.5 - half


def coefficients(half_gate, cand_in, previous, half_mix_gate, mix_gate, mix_cand):
    forget, rest = forget_and_rest(half_gate + half_mix_gate * previous)
    candidate = jnp.tanh(cand_in + mix_cand * previous)
    kept = forget * (previous - candidate)
    slopes = forget + rest * (kept * mix_gate + (mix_cand - candidate * candidate * mix_cand))
    return slopes, candidate + kept


def coefficients_at_zero(half_gate, cand_in, mix_gate, mix_cand):
    forget, rest = forget_and_rest(half_gate)
    candidate = jnp.tanh(cand_in)
    kept = forget * candidate
    slopes = forget + rest * ((mix_cand - candidate * candidate * mix_cand) - kept * mix_gate)
    return slopes, candidate - kept


def lane_part():
    return lax.broadcasted_iota(jnp.int32, (SUB, LANES), 1) // WIDE


def roll_parts(x, parts):
    parts %= PARTS
    return pltpu.roll(x, parts * WIDE, 1) if parts else x


def pack_kernel(seqs, steps, groups, gate_hbm, cand_hbm, out_hbm,
                gate_ref, cand_ref, packed, gate_flat, cand_flat, mixed, x_ref, perm_ref, in_sem, out_sem):
    rows = steps // PARTS
    owners = PARTS * SUB
    slabs = seqs * groups

    def fetch(n):
        s, lane = n // groups, pl.multiple_of((n % groups) * GROUP, GROUP)
        window = (s, slice(None), pl.ds(lane, GROUP))
        return [
            pltpu.make_async_copy(gate_hbm.at[window], gate_ref.at[n], in_sem.at[0, n]),
            pltpu.make_async_copy(cand_hbm.at[window], cand_ref.at[n], in_sem.at[1, n]),
        ]

    def store(n):
        at = pl.multiple_of(n * owners, owners)
        return pltpu.make_async_copy(packed.at[pl.ds(at, owners)], out_hbm.at[pl.ds(at, owners)], out_sem.at[n])

    for n in range(slabs):
        for copy in fetch(n):
            copy.start()

    i = lax.broadcasted_iota(jnp.int32, perm_ref.shape, 0)
    target = i % LANES // WIDE * LANES + i // LANES * WIDE + i % WIDE
    perm_ref[...] = jnp.where(lax.broadcasted_iota(jnp.int32, perm_ref.shape, 1) == target, 1.0, 0.0).astype(jnp.bfloat16)

    def gather(n, p):
        for half, (in_ref, flat) in enumerate(((gate_ref, gate_flat), (cand_ref, cand_flat))):
            for i in range(steps // SUB):
                for k in range(SUB):
                    at = (i * SUB + k) * SUB
                    flat[p, at : at + SUB, :] = in_ref[
                        n, i * SUB : (i + 1) * SUB, k * LANES : (k + 1) * LANES].astype(jnp.float32)
            for r in range(0, rows, 2):
                for u in range(PARTS):
                    two = []
                    for t in (u * rows + r, u * rows + r + 1):
                        two.append(flat[p, pl.ds(t // SUB * SUB * SUB + t % SUB, SUB, stride=SUB), :])
                    at = (half * rows + r) * SUB
                    x_ref[p, at : at + 2 * SUB, u * LANES : (u + 1) * LANES] = jnp.concatenate(
                        two, axis=0).astype(jnp.bfloat16)

    def move(p):
        moved = jnp.dot(x_ref[p], perm_ref[...], preferred_element_type=jnp.float32)
        for q in range(PARTS):
            at = q * 2 * rows * SUB
            mixed[p, at : at + 2 * rows * SUB, :] = moved[:, q * LANES : (q + 1) * LANES]

    def spread(n, p):
        for q in range(PARTS):
            for k in range(SUB):
                for g in range(rows // SUB):
                    at = (q * 2 * rows + g * 2 * SUB) * SUB + k
                    two = [mixed[p, pl.ds(at + h * SUB * SUB, SUB, stride=SUB), :] for h in range(2)]
                    packed[n * owners + q * SUB + k, g * 2 * SUB : (g + 1) * 2 * SUB, :] = jnp.concatenate(
                        two, axis=0).astype(jnp.bfloat16)
        store(n).start()

    def wait(n):
        for copy in fetch(n):
            copy.wait()

    def pair(m, _):
        for p in range(2):
            wait(2 * m + p)
        for p in range(2):
            gather(2 * m + p, p)
        for p in range(2):
            move(p)
        for p in range(2):
            spread(2 * m + p, p)
        return 0

    lax.fori_loop(0, slabs // 2, pair, 0)
    for n in range(slabs):
        store(n).wait()


def repeat_first_part(x, part):
    x = jnp.where(part == 0, x, roll_parts(x, 1))
    return jnp.where(part < 2, x, roll_parts(x, 2))


def own_row(ref, n, k, q, part):
    row = jnp.broadcast_to(ref[n, pl.ds(k, 1), :], (SUB, LANES))
    return repeat_first_part(pltpu.roll(row, ((PARTS - q) % PARTS) * WIDE, 1), part)


def owner_kernel(groups, tiles, rows, got_ref, start_ref, mg_all_ref, mc_all_ref, out_ref,
                 flat, gate_ref, cand_ref, slopes_ref, offset_ref, scale_ref, shift_ref, entry_ref):
    part = lane_part()
    sub = lax.broadcasted_iota(jnp.int32, (SUB, LANES), 0)
    owner = lax.axis_index("tm") * lax.axis_size("grp") + lax.axis_index("grp")
    n, q, k = owner // (PARTS * SUB), (owner // SUB) % PARTS, owner % SUB
    mg = own_row(mg_all_ref, n % groups, k, q, part)
    half_mg = 0.5 * mg
    mc = own_row(mc_all_ref, n % groups, k, q, part)
    start = own_row(start_ref, n, k, q, part)
    def first(pair, _):
        for p in range(2):
            v = 2 * pair + p
            head = jnp.where(jnp.logical_and(v == 0, jnp.logical_and(sub == 0, part == 0)), start, 0.0)
            for m in range(SUB):
                got = got_ref[v * SUB + m].astype(jnp.float32)
                for g in range(2 * rows // SUB):
                    at = ((p * 2 * rows) + g * SUB + m) * SUB
                    flat[at : at + SUB, :] = got[g * SUB : (g + 1) * SUB]
            for r in range(rows):
                at = (p * 2 * rows + r // SUB * SUB) * SUB + r % SUB
                g = 0.5 * flat[pl.ds(at, SUB, stride=SUB), :]
                c = flat[pl.ds(at + rows * SUB, SUB, stride=SUB), :]
                if r == 0:
                    sl, of = coefficients(g, c, head, half_mg, mg, mc)
                    of -= sl * head
                    a, b = sl, of
                else:
                    sl, of = coefficients_at_zero(g, c, mg, mc)
                    a, b = sl * a, sl * b + of
                gate_ref[v, r] = g
                cand_ref[v, r] = c
                slopes_ref[v, r] = sl
                offset_ref[v, r] = of
            scale_ref[v] = a
            shift_ref[v] = b
        return 0

    def following(last, v, _):
        e = entry_ref[v]
        for r in range(rows):
            sl, at_slope = coefficients(gate_ref[v, r], cand_ref[v, r], e, half_mg, mg, mc)
            if last:
                a, b = (sl, at_slope - sl * e) if r == 0 else (sl * a, sl * (b - e) + at_slope)
            else:
                of = at_slope - sl * e
                a, b = (sl, of) if r == 0 else (sl * a, sl * b + of)
            if r < rows - 1:
                e = slopes_ref[v, r] * e + offset_ref[v, r]
            if not last:
                slopes_ref[v, r] = sl
                offset_ref[v, r] = of
        scale_ref[v] = a
        shift_ref[v] = b
        return 0

    def scan(v, state):
        a, b = scale_ref[v], shift_ref[v]
        turned = [(roll_parts(a, step), roll_parts(b, step)) for step in range(PARTS)]
        part_a, part_b = 1.0, 0.0
        for step in (3, 2, 1):
            earlier_a = jnp.where(part >= step, turned[step][0], 1.0)
            earlier_b = jnp.where(part >= step, turned[step][1], 0.0)
            part_a, part_b = earlier_a * part_a, earlier_a * part_b + earlier_b
        a, b = a * part_a, a * part_b + b
        for step in (3, 2, 1):
            later_a = jnp.where(part < step, turned[step][0], 1.0)
            later_b = jnp.where(part < step, turned[step][1], 0.0)
            a, b = later_a * a, later_a * b + later_b
        for step in (1, 2, 4):
            earlier_a = jnp.where(sub >= step, pltpu.roll(a, step, 0), 1.0)
            earlier_b = jnp.where(sub >= step, pltpu.roll(b, step, 0), 0.0)
            a, b = a * earlier_a, a * earlier_b + b
        sub_a = jnp.where(sub >= 1, pltpu.roll(a, 1, 0), 1.0)
        sub_b = jnp.where(sub >= 1, pltpu.roll(b, 1, 0), 0.0)
        entry_ref[v] = part_a * (sub_a * state + sub_b) + part_b
        whole_a = jnp.broadcast_to(a[SUB - 1 : SUB], (SUB, LANES))
        whole_b = jnp.broadcast_to(b[SUB - 1 : SUB], (SUB, LANES))
        return whole_a * state + whole_b

    def entries(i):
        lax.fori_loop(0, tiles, scan, start, unroll=32)
        for v in range(tiles):
            at = v * SUB
            moved = roll_parts(entry_ref[v], i)
            out_ref[at : at + SUB, :] = moved if i == 0 else jnp.where(part == i, moved, out_ref[at : at + SUB, :])

    lax.fori_loop(0, tiles // 2, first, 0)
    entries(0)
    lax.fori_loop(0, tiles, functools.partial(following, False), 0, unroll=4)
    entries(1)
    lax.fori_loop(0, tiles, functools.partial(following, True), 0, unroll=4)
    entries(2)


def last_kernel(seqs, steps, groups, gate_ref, cand_ref, entry_ref, mg_ref, mc_ref, out_hbm,
                out_ref, gate_tmp, cand_tmp, out_tmp, out_sem):
    part = lane_part()

    def store(s, i):
        window = (s, pl.ds(i * SUB if isinstance(i, int) else pl.multiple_of(i * SUB, SUB), SUB))
        return pltpu.make_async_copy(out_ref.at[window], out_hbm.at[window], out_sem.at[s, i])

    at_start = jnp.logical_and(lax.axis_index("tm") == 0, lax.axis_index("grp") == 0)
    head_scale = jnp.where(at_start, 1.0, 0.0)

    def entry_rows(n):
        got = [entry_ref[(n * PARTS + q) * SUB : (n * PARTS + q + 1) * SUB, :] for q in range(PARTS)]
        rows = []
        for i in range(3):
            row = roll_parts(got[0], -i)
            for q in range(1, PARTS):
                row = jnp.where(part == q, roll_parts(got[q], q - i), row)
            rows.append(row)
        return tuple(rows)

    def block(s, i, states, begin):
        at = i * SUB if isinstance(i, int) else pl.multiple_of(i * SUB, SUB)
        done = []
        for j in range(groups):
            for k in range(SUB):
                lane = j * GROUP + k * LANES
                row = (j * SUB + k) * SUB
                gate = gate_ref[s, pl.ds(at, SUB), lane : lane + LANES].astype(jnp.float32)
                gate_tmp[row : row + SUB, :] = 0.5 * gate
                cand_tmp[row : row + SUB, :] = cand_ref[s, pl.ds(at, SUB), lane : lane + LANES].astype(jnp.float32)
        for j in range(groups):
            mg, mc = mg_ref[j], mc_ref[j]
            half_mg = 0.5 * mg
            first, second, third = states[j]
            for t in range(SUB):
                window = pl.ds(j * SUB * SUB + t, SUB, stride=SUB)
                g, c = gate_tmp[window, :], cand_tmp[window, :]
                sl2, at2 = coefficients(g, c, first, half_mg, mg, mc)
                sl3, at3 = coefficients(g, c, second, half_mg, mg, mc)
                third = sl3 * (third - second) + at3
                second = sl2 * (second - first) + at2
                if begin and t == 0:
                    head = first * head_scale
                    sl1, at1 = coefficients(g, c, head, half_mg, mg, mc)
                    first = sl1 * (first - head) + at1
                else:
                    sl1, at1 = coefficients_at_zero(g, c, mg, mc)
                    first = sl1 * first + at1
                row = (j * SUB + t) * SUB
                out_tmp[row : row + SUB, :] = third
            done.append((first, second, third))
            for k in range(SUB):
                lane = j * GROUP + k * LANES
                rows = out_tmp[pl.ds(j * SUB * SUB + k, SUB, stride=SUB), :]
                out_ref[s, pl.ds(at, SUB), lane : lane + LANES] = rows.astype(jnp.bfloat16)
        store(s, i).start()
        return tuple(done)

    for s in range(seqs):
        states = tuple(entry_rows(s * groups + j) for j in range(groups))
        states = block(s, 0, states, True)
        lax.fori_loop(1, steps // SUB, lambda i, c: block(s, i, c, False), states)
    for s in range(seqs):
        for i in range(steps // SUB):
            store(s, i).wait()


def call(kernel, outs, scratch, *args, vmem=32, space=pltpu.VMEM, out_space=None):
    spec = pl.BlockSpec(memory_space=space)
    out_spec = pl.BlockSpec(memory_space=out_space or space)
    return pl.pallas_call(
        kernel,
        out_shape=outs,
        in_specs=[spec] * len(args),
        out_specs=jax.tree.map(lambda _: out_spec, outs),
        scratch_shapes=scratch,
        compiler_params=pltpu.CompilerParams(vmem_limit_bytes=vmem * 2**20),
    )(*args)


def on_device(gate_pre, cand_pre, start_state, mix_gate, mix_cand):
    seqs, steps, width = gate_pre.shape
    groups = width // GROUP
    slabs = seqs * groups
    axes = ("tm", "grp")
    owners = lax.axis_size(axes)
    rows = steps // PARTS
    tiles = owners // SUB
    f32 = functools.partial(jax.ShapeDtypeStruct, dtype=jnp.float32)

    def scratch(*shape):
        return pltpu.VMEM(shape, jnp.float32)

    mg = mix_gate.reshape(groups, SUB, LANES)
    mc = mix_cand.reshape(groups, SUB, LANES)
    packed = call(
        functools.partial(pack_kernel, seqs, steps, groups),
        jax.ShapeDtypeStruct((owners, 2 * rows, LANES), jnp.bfloat16),
        [pltpu.VMEM((slabs, steps, GROUP), jnp.bfloat16), pltpu.VMEM((slabs, steps, GROUP), jnp.bfloat16),
         pltpu.VMEM((owners, 2 * rows, LANES), jnp.bfloat16),
         scratch(2, SUB * steps, LANES), scratch(2, SUB * steps, LANES),
         scratch(2, PARTS * 2 * rows * SUB, LANES),
         pltpu.VMEM((2, 2 * rows * SUB, PARTS * LANES), jnp.bfloat16),
         pltpu.VMEM((PARTS * LANES, PARTS * LANES), jnp.bfloat16),
         pltpu.SemaphoreType.DMA((2, slabs)), pltpu.SemaphoreType.DMA((slabs,))],
        gate_pre, cand_pre, vmem=56, space=pltpu.HBM)
    start = start_state.reshape(slabs, SUB, LANES)
    got = lax.all_to_all(packed, axes, 0, 0, tiled=True)
    tmp = scratch(groups * SUB * SUB, LANES)
    states = call(
        functools.partial(owner_kernel, groups, tiles, rows), f32((owners, LANES)),
        [scratch(2 * 2 * rows * SUB, LANES), *[scratch(tiles, rows, SUB, LANES)] * 4,
         scratch(tiles, SUB, LANES), scratch(tiles, SUB, LANES), scratch(tiles, SUB, LANES)],
        got, start, mg, mc, vmem=16)
    entry = lax.all_to_all(states.reshape(owners, 1, LANES), axes, 0, 0, tiled=True).reshape(owners, LANES)
    return call(
        functools.partial(last_kernel, seqs, steps, groups),
        jax.ShapeDtypeStruct(gate_pre.shape, jnp.bfloat16),
        [pltpu.VMEM(gate_pre.shape, jnp.bfloat16), tmp, tmp, tmp, pltpu.SemaphoreType.DMA((seqs, steps // SUB))],
        gate_pre, cand_pre, entry, mg, mc, vmem=16, out_space=pltpu.HBM)


def solution(mesh):
    time = P(None, ("tm", "grp"), None)
    return jax.shard_map(
        on_device, mesh=mesh, in_specs=(time, time, P(), P(), P()), out_specs=time, check_vma=False
    )
```

```python
import functools

import jax
import jax.numpy as jnp
from jax import lax
from jax.experimental import pallas as pl
from jax.experimental.pallas import tpu as pltpu
from jax.sharding import PartitionSpec as P

LANES = 128
SUB = 8
PARTS = 4
WIDE = LANES // PARTS
GROUP = SUB * LANES


def forget_and_rest(half_gate):
    half = 0.5 * jnp.tanh(half_gate)
    return 0.5 + half, 0.5 - half


def coefficients(half_gate, cand_in, previous, half_mix_gate, mix_gate, mix_cand):
    forget, rest = forget_and_rest(half_gate + half_mix_gate * previous)
    candidate = jnp.tanh(cand_in + mix_cand * previous)
    kept = forget * (previous - candidate)
    slopes = forget + rest * (kept * mix_gate + (mix_cand - candidate * candidate * mix_cand))
    return slopes, candidate + kept


def coefficients_at_zero(half_gate, cand_in, mix_gate, mix_cand):
    forget, rest = forget_and_rest(half_gate)
    candidate = jnp.tanh(cand_in)
    kept = forget * candidate
    slopes = forget + rest * ((mix_cand - candidate * candidate * mix_cand) - kept * mix_gate)
    return slopes, candidate - kept


def lane_part():
    return lax.broadcasted_iota(jnp.int32, (SUB, LANES), 1) // WIDE


def roll_parts(x, parts):
    parts %= PARTS
    return pltpu.roll(x, parts * WIDE, 1) if parts else x


def pack_kernel(seqs, steps, groups, gate_hbm, cand_hbm, out_hbm,
                gate_ref, cand_ref, packed, gate_flat, cand_flat, mixed, x_ref, perm_ref, in_sem, out_sem):
    rows = steps // PARTS
    owners = PARTS * SUB
    slabs = seqs * groups

    def fetch(n):
        s, lane = n // groups, pl.multiple_of((n % groups) * GROUP, GROUP)
        window = (s, slice(None), pl.ds(lane, GROUP))
        return [
            pltpu.make_async_copy(gate_hbm.at[window], gate_ref.at[n], in_sem.at[0, n]),
            pltpu.make_async_copy(cand_hbm.at[window], cand_ref.at[n], in_sem.at[1, n]),
        ]

    def store(n):
        at = pl.multiple_of(n * owners, owners)
        return pltpu.make_async_copy(packed.at[pl.ds(at, owners)], out_hbm.at[pl.ds(at, owners)], out_sem.at[n])

    for n in range(slabs):
        for copy in fetch(n):
            copy.start()

    i = lax.broadcasted_iota(jnp.int32, perm_ref.shape, 0)
    target = i % LANES // WIDE * LANES + i // LANES * WIDE + i % WIDE
    perm_ref[...] = jnp.where(lax.broadcasted_iota(jnp.int32, perm_ref.shape, 1) == target, 1.0, 0.0).astype(jnp.bfloat16)

    def gather(n, p):
        for half, (in_ref, flat) in enumerate(((gate_ref, gate_flat), (cand_ref, cand_flat))):
            for i in range(steps // SUB):
                for k in range(SUB):
                    at = (i * SUB + k) * SUB
                    flat[p, at : at + SUB, :] = in_ref[
                        n, i * SUB : (i + 1) * SUB, k * LANES : (k + 1) * LANES].astype(jnp.float32)
            for r in range(0, rows, 2):
                for u in range(PARTS):
                    two = []
                    for t in (u * rows + r, u * rows + r + 1):
                        two.append(flat[p, pl.ds(t // SUB * SUB * SUB + t % SUB, SUB, stride=SUB), :])
                    at = (half * rows + r) * SUB
                    x_ref[p, at : at + 2 * SUB, u * LANES : (u + 1) * LANES] = jnp.concatenate(
                        two, axis=0).astype(jnp.bfloat16)

    def move(p):
        moved = jnp.dot(x_ref[p], perm_ref[...], preferred_element_type=jnp.float32)
        for q in range(PARTS):
            at = q * 2 * rows * SUB
            mixed[p, at : at + 2 * rows * SUB, :] = moved[:, q * LANES : (q + 1) * LANES]

    def spread(n, p):
        for q in range(PARTS):
            for k in range(SUB):
                for g in range(rows // SUB):
                    at = (q * 2 * rows + g * 2 * SUB) * SUB + k
                    two = [mixed[p, pl.ds(at + h * SUB * SUB, SUB, stride=SUB), :] for h in range(2)]
                    packed[n * owners + q * SUB + k, g * 2 * SUB : (g + 1) * 2 * SUB, :] = jnp.concatenate(
                        two, axis=0).astype(jnp.bfloat16)
        store(n).start()

    def wait(n):
        for copy in fetch(n):
            copy.wait()

    def several(m, _):
        for p in range(4):
            wait(4 * m + p)
        for p in range(4):
            gather(4 * m + p, p)
        for p in range(4):
            move(p)
        for p in range(4):
            spread(4 * m + p, p)
        return 0

    lax.fori_loop(0, slabs // 4, several, 0)
    for n in range(slabs):
        store(n).wait()


def repeat_first_part(x, part):
    x = jnp.where(part == 0, x, roll_parts(x, 1))
    return jnp.where(part < 2, x, roll_parts(x, 2))


def own_row(ref, n, k, q, part):
    row = jnp.broadcast_to(ref[n, pl.ds(k, 1), :], (SUB, LANES))
    return repeat_first_part(pltpu.roll(row, ((PARTS - q) % PARTS) * WIDE, 1), part)


def owner_kernel(groups, tiles, rows, got_ref, start_ref, mg_all_ref, mc_all_ref, out_ref,
                 flat, gate_ref, cand_ref, slopes_ref, offset_ref, scale_ref, shift_ref, entry_ref):
    part = lane_part()
    sub = lax.broadcasted_iota(jnp.int32, (SUB, LANES), 0)
    owner = lax.axis_index("tm") * lax.axis_size("grp") + lax.axis_index("grp")
    n, q, k = owner // (PARTS * SUB), (owner // SUB) % PARTS, owner % SUB
    mg = own_row(mg_all_ref, n % groups, k, q, part)
    half_mg = 0.5 * mg
    mc = own_row(mc_all_ref, n % groups, k, q, part)
    start = own_row(start_ref, n, k, q, part)
    def first(pair, _):
        for p in range(2):
            v = 2 * pair + p
            head = jnp.where(jnp.logical_and(v == 0, jnp.logical_and(sub == 0, part == 0)), start, 0.0)
            for m in range(SUB):
                got = got_ref[v * SUB + m].astype(jnp.float32)
                for g in range(2 * rows // SUB):
                    at = ((p * 2 * rows) + g * SUB + m) * SUB
                    flat[at : at + SUB, :] = got[g * SUB : (g + 1) * SUB]
            for r in range(rows):
                at = (p * 2 * rows + r // SUB * SUB) * SUB + r % SUB
                g = 0.5 * flat[pl.ds(at, SUB, stride=SUB), :]
                c = flat[pl.ds(at + rows * SUB, SUB, stride=SUB), :]
                if r == 0:
                    sl, of = coefficients(g, c, head, half_mg, mg, mc)
                    of -= sl * head
                    a, b = sl, of
                else:
                    sl, of = coefficients_at_zero(g, c, mg, mc)
                    a, b = sl * a, sl * b + of
                gate_ref[v, r] = g
                cand_ref[v, r] = c
                slopes_ref[v, r] = sl
                offset_ref[v, r] = of
            scale_ref[v] = a
            shift_ref[v] = b
        return 0

    def following(last, v, _):
        e = entry_ref[v]
        for r in range(rows):
            sl, at_slope = coefficients(gate_ref[v, r], cand_ref[v, r], e, half_mg, mg, mc)
            if last:
                a, b = (sl, at_slope - sl * e) if r == 0 else (sl * a, sl * (b - e) + at_slope)
            else:
                of = at_slope - sl * e
                a, b = (sl, of) if r == 0 else (sl * a, sl * b + of)
            if r < rows - 1:
                e = slopes_ref[v, r] * e + offset_ref[v, r]
            if not last:
                slopes_ref[v, r] = sl
                offset_ref[v, r] = of
        scale_ref[v] = a
        shift_ref[v] = b
        return 0

    def scan(v, state):
        a, b = scale_ref[v], shift_ref[v]
        turned = [(roll_parts(a, step), roll_parts(b, step)) for step in range(PARTS)]
        part_a, part_b = 1.0, 0.0
        for step in (3, 2, 1):
            earlier_a = jnp.where(part >= step, turned[step][0], 1.0)
            earlier_b = jnp.where(part >= step, turned[step][1], 0.0)
            part_a, part_b = earlier_a * part_a, earlier_a * part_b + earlier_b
        a, b = a * part_a, a * part_b + b
        for step in (3, 2, 1):
            later_a = jnp.where(part < step, turned[step][0], 1.0)
            later_b = jnp.where(part < step, turned[step][1], 0.0)
            a, b = later_a * a, later_a * b + later_b
        for step in (1, 2, 4):
            earlier_a = jnp.where(sub >= step, pltpu.roll(a, step, 0), 1.0)
            earlier_b = jnp.where(sub >= step, pltpu.roll(b, step, 0), 0.0)
            a, b = a * earlier_a, a * earlier_b + b
        sub_a = jnp.where(sub >= 1, pltpu.roll(a, 1, 0), 1.0)
        sub_b = jnp.where(sub >= 1, pltpu.roll(b, 1, 0), 0.0)
        entry_ref[v] = part_a * (sub_a * state + sub_b) + part_b
        whole_a = jnp.broadcast_to(a[SUB - 1 : SUB], (SUB, LANES))
        whole_b = jnp.broadcast_to(b[SUB - 1 : SUB], (SUB, LANES))
        return whole_a * state + whole_b

    def entries(i):
        lax.fori_loop(0, tiles, scan, start, unroll=32)
        for v in range(tiles):
            at = v * SUB
            moved = roll_parts(entry_ref[v], i)
            out_ref[at : at + SUB, :] = moved if i == 0 else jnp.where(part == i, moved, out_ref[at : at + SUB, :])

    lax.fori_loop(0, tiles // 2, first, 0)
    entries(0)
    lax.fori_loop(0, tiles, functools.partial(following, False), 0, unroll=4)
    entries(1)
    lax.fori_loop(0, tiles, functools.partial(following, True), 0, unroll=4)
    entries(2)


def last_kernel(seqs, steps, groups, gate_ref, cand_ref, entry_ref, mg_ref, mc_ref, out_hbm,
                out_ref, gate_tmp, cand_tmp, out_tmp, out_sem):
    part = lane_part()

    def store(s, i):
        window = (s, pl.ds(i * SUB if isinstance(i, int) else pl.multiple_of(i * SUB, SUB), SUB))
        return pltpu.make_async_copy(out_ref.at[window], out_hbm.at[window], out_sem.at[s, i])

    at_start = jnp.logical_and(lax.axis_index("tm") == 0, lax.axis_index("grp") == 0)
    head_scale = jnp.where(at_start, 1.0, 0.0)

    def entry_rows(n):
        got = [entry_ref[(n * PARTS + q) * SUB : (n * PARTS + q + 1) * SUB, :] for q in range(PARTS)]
        rows = []
        for i in range(3):
            row = roll_parts(got[0], -i)
            for q in range(1, PARTS):
                row = jnp.where(part == q, roll_parts(got[q], q - i), row)
            rows.append(row)
        return tuple(rows)

    def block(s, i, states, begin):
        at = i * SUB if isinstance(i, int) else pl.multiple_of(i * SUB, SUB)
        done = []
        for j in range(groups):
            for k in range(SUB):
                lane = j * GROUP + k * LANES
                row = (j * SUB + k) * SUB
                gate = gate_ref[s, pl.ds(at, SUB), lane : lane + LANES].astype(jnp.float32)
                gate_tmp[row : row + SUB, :] = 0.5 * gate
                cand_tmp[row : row + SUB, :] = cand_ref[s, pl.ds(at, SUB), lane : lane + LANES].astype(jnp.float32)
        for j in range(groups):
            mg, mc = mg_ref[j], mc_ref[j]
            half_mg = 0.5 * mg
            first, second, third = states[j]
            for t in range(SUB):
                window = pl.ds(j * SUB * SUB + t, SUB, stride=SUB)
                g, c = gate_tmp[window, :], cand_tmp[window, :]
                sl2, at2 = coefficients(g, c, first, half_mg, mg, mc)
                sl3, at3 = coefficients(g, c, second, half_mg, mg, mc)
                third = sl3 * (third - second) + at3
                second = sl2 * (second - first) + at2
                if begin and t == 0:
                    head = first * head_scale
                    sl1, at1 = coefficients(g, c, head, half_mg, mg, mc)
                    first = sl1 * (first - head) + at1
                else:
                    sl1, at1 = coefficients_at_zero(g, c, mg, mc)
                    first = sl1 * first + at1
                row = (j * SUB + t) * SUB
                out_tmp[row : row + SUB, :] = third
            done.append((first, second, third))
            for k in range(SUB):
                lane = j * GROUP + k * LANES
                rows = out_tmp[pl.ds(j * SUB * SUB + k, SUB, stride=SUB), :]
                out_ref[s, pl.ds(at, SUB), lane : lane + LANES] = rows.astype(jnp.bfloat16)
        store(s, i).start()
        return tuple(done)

    for s in range(seqs):
        states = tuple(entry_rows(s * groups + j) for j in range(groups))
        states = block(s, 0, states, True)
        lax.fori_loop(1, steps // SUB, lambda i, c: block(s, i, c, False), states)
    for s in range(seqs):
        for i in range(steps // SUB):
            store(s, i).wait()


def call(kernel, outs, scratch, *args, vmem=32, space=pltpu.VMEM, out_space=None):
    spec = pl.BlockSpec(memory_space=space)
    out_spec = pl.BlockSpec(memory_space=out_space or space)
    return pl.pallas_call(
        kernel,
        out_shape=outs,
        in_specs=[spec] * len(args),
        out_specs=jax.tree.map(lambda _: out_spec, outs),
        scratch_shapes=scratch,
        compiler_params=pltpu.CompilerParams(vmem_limit_bytes=vmem * 2**20),
    )(*args)


def on_device(gate_pre, cand_pre, start_state, mix_gate, mix_cand):
    seqs, steps, width = gate_pre.shape
    groups = width // GROUP
    slabs = seqs * groups
    axes = ("tm", "grp")
    owners = lax.axis_size(axes)
    rows = steps // PARTS
    tiles = owners // SUB
    f32 = functools.partial(jax.ShapeDtypeStruct, dtype=jnp.float32)

    def scratch(*shape):
        return pltpu.VMEM(shape, jnp.float32)

    mg = mix_gate.reshape(groups, SUB, LANES)
    mc = mix_cand.reshape(groups, SUB, LANES)
    packed = call(
        functools.partial(pack_kernel, seqs, steps, groups),
        jax.ShapeDtypeStruct((owners, 2 * rows, LANES), jnp.bfloat16),
        [pltpu.VMEM((slabs, steps, GROUP), jnp.bfloat16), pltpu.VMEM((slabs, steps, GROUP), jnp.bfloat16),
         pltpu.VMEM((owners, 2 * rows, LANES), jnp.bfloat16),
         scratch(4, SUB * steps, LANES), scratch(4, SUB * steps, LANES),
         scratch(4, PARTS * 2 * rows * SUB, LANES),
         pltpu.VMEM((4, 2 * rows * SUB, PARTS * LANES), jnp.bfloat16),
         pltpu.VMEM((PARTS * LANES, PARTS * LANES), jnp.bfloat16),
         pltpu.SemaphoreType.DMA((2, slabs)), pltpu.SemaphoreType.DMA((slabs,))],
        gate_pre, cand_pre, vmem=56, space=pltpu.HBM)
    start = start_state.reshape(slabs, SUB, LANES)
    got = lax.all_to_all(packed, axes, 0, 0, tiled=True)
    tmp = scratch(groups * SUB * SUB, LANES)
    states = call(
        functools.partial(owner_kernel, groups, tiles, rows), f32((owners, LANES)),
        [scratch(2 * 2 * rows * SUB, LANES), *[scratch(tiles, rows, SUB, LANES)] * 4,
         scratch(tiles, SUB, LANES), scratch(tiles, SUB, LANES), scratch(tiles, SUB, LANES)],
        got, start, mg, mc, vmem=16)
    entry = lax.all_to_all(states.reshape(owners, 1, LANES), axes, 0, 0, tiled=True).reshape(owners, LANES)
    return call(
        functools.partial(last_kernel, seqs, steps, groups),
        jax.ShapeDtypeStruct(gate_pre.shape, jnp.bfloat16),
        [pltpu.VMEM(gate_pre.shape, jnp.bfloat16), tmp, tmp, tmp, pltpu.SemaphoreType.DMA((seqs, steps // SUB))],
        gate_pre, cand_pre, entry, mg, mc, vmem=16, out_space=pltpu.HBM)


def solution(mesh):
    time = P(None, ("tm", "grp"), None)
    return jax.shard_map(
        on_device, mesh=mesh, in_specs=(time, time, P(), P(), P()), out_specs=time, check_vma=False
    )
```
